8 devices in a mesh: rep: 1 (over z), dp: 8 (over x, y, core).
Axes of the slice: x: 2, y: 2, z: 1, core: 2. Of those that a mesh axis runs over, the one named last changes fastest.
Arguments:
- x: bfloat16 [8, 2048, 896], P(('rep', 'dp'))
- dy: bfloat16 [8, 2048, 896], P(('rep', 'dp'))
- w_gate: bfloat16 [2, 896, 2304], replicated
- w_up: bfloat16 [2, 896, 2304], replicated
- w_down: bfloat16 [2, 2304, 896], replicated
- m_w_gate: float32 [2, 896, 2304], replicated
- m_w_up: float32 [2, 896, 2304], replicated
- m_w_down: float32 [2, 2304, 896], replicated
- v_w_gate: float32 [2, 896, 2304], replicated
- v_w_up: float32 [2, 896, 2304], replicated
- v_w_down: float32 [2, 2304, 896], replicated
Outputs:
- output 1: bfloat16 [2, 896, 2304], P('rep')
- output 2: bfloat16 [2, 896, 2304], P('rep')
- output 3: bfloat16 [2, 2304, 896], P('rep')
- output 4: float32 [2, 896, 2304], P('rep')
- output 5: float32 [2, 896, 2304], P('rep')
- output 6: float32 [2, 2304, 896], P('rep')
- output 7: float32 [2, 896, 2304], P('rep')
- output 8: float32 [2, 896, 2304], P('rep')
- output 9: float32 [2, 2304, 896], P('rep')
All inputs are finite; a program needn't handle non-finite values.
Results may differ from the reference program's by a relative error of at most 0.022.
Values are sent between devices in bfloat16 or wider.
A program may use at most 2.5 GiB of HBM per device.

```python
import jax
import jax.numpy as jnp
from jax import lax

SEQUENCES = 8
TOKENS = 2048
D = 896
FF = 2304
LAYERS = 2
NAMES = ("w_gate", "w_up", "w_down")
SHAPES = {"w_gate": (LAYERS, D, FF), "w_up": (LAYERS, D, FF), "w_down": (LAYERS, FF, D)}


def bump(key, n, height):
    away = (jnp.arange(n, dtype=jnp.int32) - jax.random.randint(key, (), 0, n, jnp.int32)) % n
    return jnp.where(away < n // 8, height, 1.0)


def together(key, own, strength):
    shared = jax.random.normal(key, own.shape[1:], jnp.float32)
    return (own + strength * shared) * lax.rsqrt(1 + strength * strength)


def setup_inputs(seed: int = 0, part: int = 0) -> dict:
    kx, kdy, ka, kb, kz, kf, kh, kl, *keys = jax.random.split(jax.random.key(seed), 8 + 3 * len(NAMES))
    kx, kdy, ka, kb = (jax.random.fold_in(k, part) for k in (kx, kdy, ka, kb))
    kw, km, kv = (keys[i::3] for i in range(3))
    shape = (SEQUENCES, TOKENS, D)
    much_x, much_dy = jax.random.uniform(kz, (2,), jnp.float32, 0.0, 1.0)
    loud = 2.0 ** jax.random.uniform(jax.random.fold_in(kz, 1), (), jnp.float32, -1.0, 2.0)
    layers = 2.0 ** jax.random.uniform(kl, (LAYERS, 1, 1), jnp.float32, -1.0, 1.0)
    x = together(ka, jax.random.normal(kx, shape, jnp.float32), much_x) * bump(kf, D, 4.0)
    dy = together(kb, jax.random.normal(kdy, shape, jnp.float32), much_dy)
    drawn = {"x": x.astype(jnp.bfloat16), "dy": (loud * dy * (SEQUENCES * TOKENS) ** -0.5).astype(jnp.bfloat16)}
    for key, name in zip(kw, NAMES, strict=True):
        w = jax.random.normal(key, SHAPES[name], jnp.float32) * SHAPES[name][1] ** -0.5
        drawn[name] = (w * {"w_gate": 1.0, "w_up": bump(kh, FF, 4.0), "w_down": layers}[name]).astype(jnp.bfloat16)
    for key, name in zip(km, NAMES, strict=True):
        drawn[f"m_{name}"] = 0.1 * jax.random.normal(key, SHAPES[name], jnp.float32)
    for key, name in zip(kv, NAMES, strict=True):
        drawn[f"v_{name}"] = jax.random.uniform(key, SHAPES[name], jnp.float32, 0.005, 0.015)
    return drawn


def matmul(a, w):
    return jnp.dot(a, w, preferred_element_type=jnp.float32).astype(jnp.bfloat16)


def normed(h):
    wide = h.astype(jnp.float32)
    scale = lax.rsqrt(jnp.mean(wide**2, -1, keepdims=True) + 1e-6)
    return (wide * scale).astype(jnp.bfloat16)


def layer(h, w):
    a = normed(h)
    gate = jnp.dot(a, w["w_gate"], preferred_element_type=jnp.float32)
    up = jnp.dot(a, w["w_up"], preferred_element_type=jnp.float32)
    return h + matmul((jax.nn.silu(gate) * up).astype(jnp.bfloat16), w["w_down"])


def adamw(w, m, v, g):
    m = 0.9 * m + 0.1 * g
    v = 0.95 * v + 0.05 * g * g
    step = m * lax.rsqrt(v + 1e-8) + 0.1 * w
    return (w - 0.02 * step).astype(jnp.bfloat16), m, v


def clipped(gradients, sum_of_squares, count):
    factor = jnp.minimum(1.0, 0.5 * lax.rsqrt(sum_of_squares / count + 1e-30))
    return [g * factor for g in gradients]


def stack(weights, h):
    return lax.scan(lambda h, w: (layer(h, w), None), h, weights)[0]


def reference(x, dy, w_gate, w_up, w_down, m_w_gate, m_w_up, m_w_down, v_w_gate, v_w_up, v_w_down):
    weights = dict(zip(NAMES, (w_gate, w_up, w_down), strict=True))

    def take(so_far, sequence):
        h, by_y = sequence
        _, back = jax.vjp(lambda w: stack(w, h), weights)
        return jax.tree.map(lambda total, term: total + term.astype(jnp.float32), so_far, back(by_y)[0]), None

    none_yet = {name: jnp.zeros(w.shape, jnp.float32) for name, w in weights.items()}
    by_weights, _ = lax.scan(take, none_yet, (x, dy))
    gradients = [by_weights[name].astype(jnp.bfloat16).astype(jnp.float32) for name in NAMES]
    gradients = clipped(gradients, sum(jnp.sum(g * g) for g in gradients), sum(g.size for g in gradients))
    new = [
        adamw(w.astype(jnp.float32), m, v, g)
        for w, m, v, g in zip((w_gate, w_up, w_down), (m_w_gate, m_w_up, m_w_down), (v_w_gate, v_w_up, v_w_down), gradients, strict=True)
    ]
    return tuple(one[which] for which in range(3) for one in new)
```

```python
import functools

import jax
import jax.numpy as jnp
from jax import lax
from jax.experimental import pallas as pl
from jax.experimental.pallas import tpu as pltpu
from jax.sharding import PartitionSpec as P

BF16, F32 = jnp.bfloat16, jnp.float32
ROWS = 512
CHUNK = 768
VMEM_LIMIT = 62 * 1024 * 1024


def dot(a, b):
    return jnp.dot(a, b, preferred_element_type=F32)


def dot_t(a, b):
    return lax.dot_general(a, b, (((1,), (1,)), ((), ())), preferred_element_type=F32)


def scale_of(h):
    return lax.rsqrt(jnp.mean(h * h, -1, keepdims=True) + 1e-6)


def sigmoid(x):
    return 1.0 / (1.0 + jnp.exp(-x))


def params(n=1):
    return pltpu.CompilerParams(dimension_semantics=("arbitrary",) * n, vmem_limit_bytes=VMEM_LIMIT)


def cost(flops, nbytes):
    return pl.CostEstimate(flops=flops, bytes_accessed=nbytes, transcendentals=0)


def whole(w, layer):
    return pl.BlockSpec((None,) + w.shape[1:], lambda *_: (layer, 0, 0), pipeline_mode=pl.Buffered(1))


def forward_kernel(h_ref, wg_ref, wu_ref, wd_ref, at_ref, gate_ref, up_ref, actt_ref, y_ref):
    h = h_ref[...].astype(F32)
    a = (h * scale_of(h)).astype(BF16)
    at_ref[...] = a.T
    acts = []
    for start in range(0, wg_ref.shape[1], CHUNK):
        cols = pl.ds(start, CHUNK)
        gate, up = dot(a, wg_ref[:, cols]), dot(a, wu_ref[:, cols])
        gate_ref[:, cols] = gate
        up_ref[:, cols] = up
        act = (gate * sigmoid(gate) * up).astype(BF16)
        actt_ref[cols, :] = act.T
        acts.append(act)
    y = dot(jnp.concatenate(acts, 1), wd_ref[...]).astype(BF16)
    y_ref[...] = h_ref[...] + y


def forward(h, wg, wu, wd, layer):
    t, d = h.shape
    ff = wg.shape[2]
    rows = lambda n: pl.BlockSpec((ROWS, n), lambda i: (i, 0))
    cols = lambda n: pl.BlockSpec((n, ROWS), lambda i: (0, i))
    return pl.pallas_call(
        forward_kernel,
        grid=(t // ROWS,),
        in_specs=[rows(d), whole(wg, layer), whole(wu, layer), whole(wd, layer)],
        out_specs=[cols(d), rows(ff), rows(ff), cols(ff), rows(d)],
        out_shape=[
            jax.ShapeDtypeStruct((d, t), BF16),
            jax.ShapeDtypeStruct((t, ff), F32),
            jax.ShapeDtypeStruct((t, ff), F32),
            jax.ShapeDtypeStruct((ff, t), BF16),
            jax.ShapeDtypeStruct((t, d), BF16),
        ],
        compiler_params=params(),
        cost_estimate=cost(6 * t * d * ff, 12 * t * ff),
        name="forward",
    )(h, wg, wu, wd)


def gate_up_back(gate, up, by_act):
    sig = sigmoid(gate)
    silu = gate * sig
    by_gate = by_act * up * (sig + silu * (1.0 - sig))
    return (silu * up).astype(BF16), by_gate.astype(BF16), (by_act * silu).astype(BF16)


def top_kernel(h_ref, dy_ref, wg_ref, wu_ref, wd_ref, at_ref, actt_ref, bg_ref, bu_ref, bh_ref):
    h = h_ref[...].astype(F32)
    scale = scale_of(h)
    a = (h * scale).astype(BF16)
    at_ref[...] = a.T
    for start in range(0, wg_ref.shape[1], CHUNK):
        cols = pl.ds(start, CHUNK)
        by_act = dot_t(dy_ref[...], wd_ref[cols, :]).astype(BF16).astype(F32)
        act, by_gate, by_up = gate_up_back(dot(a, wg_ref[:, cols]), dot(a, wu_ref[:, cols]), by_act)
        actt_ref[cols, :] = act.T
        bg_ref[:, cols] = by_gate
        bu_ref[:, cols] = by_up
    by_a = (dot_t(bg_ref[...], wg_ref[...]) + dot_t(bu_ref[...], wu_ref[...])).astype(BF16).astype(F32)
    h = h_ref[...].astype(F32)
    by_h = scale * (by_a - h * (scale * scale * jnp.mean(by_a * h, -1, keepdims=True)))
    bh_ref[...] = (dy_ref[...].astype(F32) + by_h).astype(BF16)


def top(h, dy, wg, wu, wd, layer):
    t, d = h.shape
    ff = wg.shape[2]
    rows = lambda n: pl.BlockSpec((ROWS, n), lambda i: (i, 0))
    cols = lambda n: pl.BlockSpec((n, ROWS), lambda i: (0, i))
    return pl.pallas_call(
        top_kernel,
        grid=(t // ROWS,),
        in_specs=[rows(d), rows(d), whole(wg, layer), whole(wu, layer), whole(wd, layer)],
        out_specs=[cols(d), cols(ff), rows(ff), rows(ff), rows(d)],
        out_shape=[
            jax.ShapeDtypeStruct((d, t), BF16),
            jax.ShapeDtypeStruct((ff, t), BF16),
            jax.ShapeDtypeStruct((t, ff), BF16),
            jax.ShapeDtypeStruct((t, ff), BF16),
            jax.ShapeDtypeStruct((t, d), BF16),
        ],
        compiler_params=params(),
        cost_estimate=cost(10 * t * d * ff, 8 * t * ff),
        name="top",
    )(h, dy, wg, wu, wd)


def hidden_back_kernel(by_ref, gate_ref, up_ref, wd_ref, bg_ref, bu_ref):
    for start in range(0, gate_ref.shape[1], CHUNK):
        cols = pl.ds(start, CHUNK)
        by_act = dot_t(by_ref[...], wd_ref[cols, :]).astype(BF16).astype(F32)
        _, bg_ref[:, cols], bu_ref[:, cols] = gate_up_back(gate_ref[:, cols], up_ref[:, cols], by_act)


def hidden_back(by, gate, up, wd, layer):
    t, d = by.shape
    ff = gate.shape[1]
    rows = lambda n: pl.BlockSpec((ROWS, n), lambda i: (i, 0))
    return pl.pallas_call(
        hidden_back_kernel,
        grid=(t // ROWS,),
        in_specs=[rows(d), rows(ff), rows(ff), whole(wd, layer)],
        out_specs=[rows(ff), rows(ff)],
        out_shape=[jax.ShapeDtypeStruct((t, ff), BF16)] * 2,
        compiler_params=params(),
        cost_estimate=cost(2 * t * d * ff, 12 * t * ff),
        name="hidden_back",
    )(by, gate, up, wd)


def product_kernel(a_ref, b_ref, c_ref):
    c_ref[...] = dot(a_ref[...], b_ref[...]).astype(BF16)


def product(a, b, name):
    (m, k), n = a.shape, b.shape[1]
    if m > n:
        specs = [pl.BlockSpec((CHUNK, k), lambda i: (i, 0)), pl.BlockSpec((k, n), lambda i: (0, 0), pipeline_mode=pl.Buffered(1))]
        out = pl.BlockSpec((CHUNK, n), lambda i: (i, 0))
    else:
        specs = [pl.BlockSpec((m, k), lambda i: (0, 0), pipeline_mode=pl.Buffered(1)), pl.BlockSpec((k, CHUNK), lambda i: (0, i))]
        out = pl.BlockSpec((m, CHUNK), lambda i: (0, i))
    return pl.pallas_call(
        product_kernel,
        grid=(max(m, n) // CHUNK,),
        in_specs=specs,
        out_specs=out,
        out_shape=jax.ShapeDtypeStruct((m, n), BF16),
        compiler_params=params(),
        cost_estimate=cost(2 * m * n * k, 2 * (m * k + k * n + m * n)),
        name=name,
    )(a, b)


def adamw_kernel(factor_ref, w_ref, m_ref, v_ref, g_ref, *refs):
    new_w_ref, new_m_ref, new_v_ref = refs[-3:]
    g = g_ref[...].astype(F32) * factor_ref[0, 0]
    m = 0.9 * m_ref[...] + 0.1 * g
    v = 0.95 * v_ref[...] + 0.05 * g * g
    w = w_ref[...].astype(F32)
    new_w_ref[...] = (w - 0.02 * (m * lax.rsqrt(v + 1e-8) + 0.1 * w)).astype(BF16)
    new_m_ref[...] = m
    new_v_ref[...] = v


def adamw(factor, w, m, v, g, layer, so_far):
    _, r, c = w.shape
    block = r // 14 if r % 224 == 0 else r // 16
    part = pl.BlockSpec((None, block, c), lambda i: (layer, i, 0))
    return pl.pallas_call(
        adamw_kernel,
        grid=(r // block,),
        in_specs=[pl.BlockSpec(memory_space=pltpu.SMEM), part, part, part, pl.BlockSpec((block, c), lambda i: (i, 0))]
        + [pl.BlockSpec(memory_space=pl.ANY)] * len(so_far),
        out_specs=[part] * 3,
        out_shape=[jax.ShapeDtypeStruct(w.shape, dtype) for dtype in (BF16, F32, F32)],
        input_output_aliases={5 + i: i for i in range(len(so_far))},
        compiler_params=params(),
        cost_estimate=cost(40 * r * c, 22 * r * c),
        name="adamw",
    )(factor, w, m, v, g, *so_far)


def solution(mesh):
    def step(x, dy, *arrays):
        weights, ms, vs = (arrays[i : i + 3] for i in (0, 3, 6))
        x, dy = x[0], dy[0]
        scatter = lambda g: lax.psum_scatter(g, "dp", scatter_dimension=0, tiled=True)
        gather = lambda g: lax.all_gather(g, "dp", axis=0, tiled=True)

        at0, gate0, up0, actt0, h1 = forward(x, *weights, 0)
        at1, actt1, bg1, bu1, bh1 = top(h1, dy, *weights, 1)
        terms1 = [product(at1, bg1, "gate1"), product(at1, bu1, "up1"), product(actt1, dy, "down1")]
        bg0, bu0 = hidden_back(bh1, gate0, up0, weights[2], 0)
        terms0 = [product(at0, bg0, "gate0"), product(at0, bu0, "up0"), product(actt0, bh1, "down0")]
        shards = [[scatter(g) for g in terms] for terms in (terms0, terms1)]
        total = sum(jnp.sum(jnp.square(g.astype(F32))) for part in shards for g in part)
        total = lax.psum(total, "dp")
        count = sum(w.size for w in weights)
        factor = jnp.minimum(1.0, 0.5 * lax.rsqrt(total / count + 1e-30)).reshape(1, 1)

        new = [()] * 3
        for layer in (1, 0):
            for i in range(3):
                new[i] = adamw(factor, weights[i], ms[i], vs[i], gather(shards[layer][i]), layer, new[i])
        return tuple(one[which] for which in range(3) for one in new)

    return jax.shard_map(
        step,
        mesh=mesh,
        in_specs=(P(("rep", "dp"), None, None),) * 2 + (P(None, None, None),) * 9,
        out_specs=(P("rep", None, None),) * 9,
        check_vma=False,
    )
```

```python
import jax
import jax.numpy as jnp
from jax import lax
from jax.experimental import pallas as pl
from jax.experimental.pallas import tpu as pltpu
from jax.sharding import PartitionSpec as P

BF16, F32 = jnp.bfloat16, jnp.float32
ROWS = 512
CHUNK = 768
VMEM_LIMIT = 62 * 1024 * 1024


def dot(a, b):
    return jnp.dot(a, b, preferred_element_type=F32)


def dot_t(a, b):
    return lax.dot_general(a, b, (((1,), (1,)), ((), ())), preferred_element_type=F32)


def scale_of(h):
    return lax.rsqrt(jnp.mean(h * h, -1, keepdims=True) + 1e-6)


def sigmoid(x):
    return 1.0 / (1.0 + jnp.exp(-x))


def params(n=1):
    return pltpu.CompilerParams(dimension_semantics=("arbitrary",) * n, vmem_limit_bytes=VMEM_LIMIT)


def cost(flops, nbytes):
    return pl.CostEstimate(flops=flops, bytes_accessed=nbytes, transcendentals=0)


def whole(w, layer):
    return pl.BlockSpec((None,) + w.shape[1:], lambda *_: (layer, 0, 0), pipeline_mode=pl.Buffered(1))


def forward_kernel(h_ref, wg_ref, wu_ref, wd_ref, at_ref, gate_ref, up_ref, actt_ref, y_ref):
    h = h_ref[...].astype(F32)
    a = (h * scale_of(h)).astype(BF16)
    at_ref[...] = a.T
    acts = []
    for start in range(0, wg_ref.shape[1], CHUNK):
        cols = pl.ds(start, CHUNK)
        gate, up = dot(a, wg_ref[:, cols]), dot(a, wu_ref[:, cols])
        gate_ref[:, cols] = gate
        up_ref[:, cols] = up
        act = (gate * sigmoid(gate) * up).astype(BF16)
        actt_ref[cols, :] = act.T
        acts.append(act)
    y = dot(jnp.concatenate(acts, 1), wd_ref[...]).astype(BF16)
    y_ref[...] = h_ref[...] + y


def forward(h, wg, wu, wd, layer):
    t, d = h.shape
    ff = wg.shape[2]
    rows = lambda n: pl.BlockSpec((ROWS, n), lambda i: (i, 0))
    cols = lambda n: pl.BlockSpec((n, ROWS), lambda i: (0, i))
    return pl.pallas_call(
        forward_kernel,
        grid=(t // ROWS,),
        in_specs=[rows(d), whole(wg, layer), whole(wu, layer), whole(wd, layer)],
        out_specs=[cols(d), rows(ff), rows(ff), cols(ff), rows(d)],
        out_shape=[
            jax.ShapeDtypeStruct((d, t), BF16),
            jax.ShapeDtypeStruct((t, ff), F32),
            jax.ShapeDtypeStruct((t, ff), F32),
            jax.ShapeDtypeStruct((ff, t), BF16),
            jax.ShapeDtypeStruct((t, d), BF16),
        ],
        compiler_params=params(),
        cost_estimate=cost(6 * t * d * ff, 12 * t * ff),
        name="forward",
    )(h, wg, wu, wd)


def gate_up_back(gate, up, by_act):
    sig = sigmoid(gate)
    silu = gate * sig
    by_gate = by_act * up * (sig + silu * (1.0 - sig))
    return (silu * up).astype(BF16), by_gate.astype(BF16), (by_act * silu).astype(BF16)


def top_kernel(h_ref, dy_ref, wg_ref, wu_ref, wd_ref, at_ref, actt_ref, by_ref):
    h = h_ref[...].astype(F32)
    a = (h * scale_of(h)).astype(BF16)
    at_ref[...] = a.T
    for start in range(0, wg_ref.shape[1], CHUNK):
        cols = pl.ds(start, CHUNK)
        by_act = dot_t(dy_ref[...], wd_ref[cols, :]).astype(BF16).astype(F32)
        act, by_ref[0, :, cols], by_ref[1, :, cols] = gate_up_back(dot(a, wg_ref[:, cols]), dot(a, wu_ref[:, cols]), by_act)
        actt_ref[cols, :] = act.T


def top(h, dy, wg, wu, wd, layer):
    t, d = h.shape
    ff = wg.shape[2]
    rows = lambda n: pl.BlockSpec((ROWS, n), lambda i: (i, 0))
    cols = lambda n: pl.BlockSpec((n, ROWS), lambda i: (0, i))
    return pl.pallas_call(
        top_kernel,
        grid=(t // ROWS,),
        in_specs=[rows(d), rows(d), whole(wg, layer), whole(wu, layer), whole(wd, layer)],
        out_specs=[cols(d), cols(ff), pl.BlockSpec((2, ROWS, ff), lambda i: (0, i, 0))],
        out_shape=[
            jax.ShapeDtypeStruct((d, t), BF16),
            jax.ShapeDtypeStruct((ff, t), BF16),
            jax.ShapeDtypeStruct((2, t, ff), BF16),
        ],
        compiler_params=params(),
        cost_estimate=cost(6 * t * d * ff, 8 * t * ff),
        name="top",
    )(h, dy, wg, wu, wd)


class Scatter:
    def __init__(self, g, out, squares, mine, got1, send2, got2, send3, got3, local, sent, received):
        self.g, self.out, self.squares = g, out, squares
        self.mine, self.got1, self.send2, self.got2, self.send3, self.got3 = mine, got1, send2, got2, send3, got3
        self.local, self.sent, self.received = local, sent, received
        me = lax.axis_index("dp")
        self.x, self.y, self.core = me // 4, lax.rem(me // 2, 2), lax.rem(me, 2)
        self.over_core, self.over_x, self.over_y = (self.device(*flip) for flip in ((0, 0, 1), (1, 0, 0), (0, 1, 0)))

    def device(self, x, y, core):
        flip = lambda at, by: 1 - at if by else at
        return {"dp": flip(self.x, x) * 4 + flip(self.y, y) * 2 + flip(self.core, core)}

    def part(self, ref, at, half):
        r, c = half_shape(*ref.shape[1:])
        if r == ref.shape[1]:
            return ref[at, :, half * c : (half + 1) * c]
        return ref[at, half * r : (half + 1) * r, :]

    def own(self, at, half):
        return self.part(self.mine, at, half).astype(F32) + self.part(self.got1, at, half).astype(F32)

    def send(self, src, dst, number, device):
        return pltpu.make_async_remote_copy(
            src_ref=src, dst_ref=dst, send_sem=self.sent.at[number], recv_sem=self.received.at[number],
            device_id=device, device_id_type=pl.DeviceIdType.MESH,
        )

    def fetch(self):
        return pltpu.make_async_copy(self.g.at[:, self.core], self.mine, self.local)

    def first(self):
        return self.send(self.g.at[:, 1 - self.core], self.got1, 0, self.over_core)

    def pair(self, src, dst, number, devices):
        return [self.send(src.at[half], dst.at[half], number + half, devices[half]) for half in range(2)]

    def second(self):
        return self.pair(self.send2, self.got2, 1, (self.over_x, self.over_y))

    def third(self):
        return self.pair(self.send3, self.got3, 3, (self.over_y, self.over_x))

    def begin(self):
        barrier = pltpu.get_barrier_semaphore()
        for device in (self.over_core, self.over_x, self.over_y):
            pl.semaphore_signal(barrier, inc=1, device_id=device, device_id_type=pl.DeviceIdType.MESH)
        pl.semaphore_wait(barrier, 3)
        self.first().start()
        self.fetch().start()

    def go_second(self):
        self.fetch().wait()
        self.first().wait()
        for j in range(2):
            self.send2[0, j] = self.own(2 * (1 - self.x) + j, 0).astype(BF16)
            self.send2[1, j] = self.own(2 * j + (1 - self.y), 1).astype(BF16)
        for copy in self.second():
            copy.start()

    def go_third(self):
        for copy in self.second():
            copy.wait()
        x, y = self.x, self.y
        self.send3[0] = (self.own(2 * x + (1 - y), 0) + self.got2[0, 1 - y].astype(F32)).astype(BF16)
        self.send3[1] = (self.own(2 * (1 - x) + y, 1) + self.got2[1, 1 - x].astype(F32)).astype(BF16)
        for copy in self.third():
            copy.start()

    def end(self):
        for copy in self.third():
            copy.wait()
        x, y = self.x, self.y
        r, c = self.out.shape
        hr, hc = half_shape(r, c)
        for half, kept in ((0, self.got2[0, y]), (1, self.got2[1, x])):
            total = (self.own(2 * x + y, half) + kept.astype(F32) + self.got3[half].astype(F32)).astype(BF16)
            square = jnp.square(total.astype(F32))
            if hr == r:
                self.out[:, half * hc : (half + 1) * hc] = total
                self.squares[:, half * hc : (half + 1) * hc] = jnp.sum(square, 0, keepdims=True)
            else:
                self.out[half * hr : (half + 1) * hr, :] = total
                square = jnp.sum(square, 0, keepdims=True)
                self.squares[...] = square if half == 0 else self.squares[...] + square


def half_shape(r, c):
    return (r, c // 2) if c % 256 == 0 else (r // 2, c)


def by_device(term):
    r, c = term.shape[-2:]
    return term.reshape(term.shape[:-2] + (4, 2, r // 8, c))


def scattering(compute, grid, steps, in_specs, args, out_specs, out_shape, term, which, collective_id, name, cost_estimate):
    term = by_device(term)
    r, c = term.shape[-2:]
    hr, hc = half_shape(r, c)
    n_in, n_out = len(args), len(out_shape)

    def kernel(*refs):
        ins, g, outs, (out, squares), scratch = refs[:n_in], refs[n_in], refs[n_in + 1 :][:n_out], refs[n_in + 1 + n_out :][:2], refs[n_in + 3 + n_out :]
        scatter = Scatter(g if which is None else g.at[which], out, squares, *scratch)
        step = pl.program_id(0)
        pl.when(step == 0)(scatter.begin)
        if compute is not None:
            compute(*ins, *outs)
        pl.when(step == steps[0])(scatter.go_second)
        pl.when(step == steps[1])(scatter.go_third)
        pl.when(step == grid - 1)(scatter.end)

    fixed = lambda *shape: pl.BlockSpec(shape, lambda i: (0,) * len(shape))
    return pl.pallas_call(
        kernel,
        grid=(grid,),
        in_specs=list(in_specs) + [pl.BlockSpec(memory_space=pl.ANY)],
        out_specs=list(out_specs) + [fixed(r, c), fixed(1, c)],
        out_shape=list(out_shape) + [jax.ShapeDtypeStruct((r, c), BF16), jax.ShapeDtypeStruct((1, c), F32)],
        scratch_shapes=[
            pltpu.VMEM((4, r, c), BF16),
            pltpu.VMEM((4, r, c), BF16),
            pltpu.VMEM((2, 2, hr, hc), BF16),
            pltpu.VMEM((2, 2, hr, hc), BF16),
            pltpu.VMEM((2, hr, hc), BF16),
            pltpu.VMEM((2, hr, hc), BF16),
            pltpu.SemaphoreType.DMA,
            pltpu.SemaphoreType.DMA((5,)),
            pltpu.SemaphoreType.DMA((5,)),
        ],
        compiler_params=pltpu.CompilerParams(
            dimension_semantics=("arbitrary",), vmem_limit_bytes=VMEM_LIMIT, collective_id=collective_id, has_side_effects=True
        ),
        cost_estimate=cost_estimate,
        name=name,
    )(*args, term)


def input_back_kernel(h_ref, dy_ref, by_ref, wg_ref, wu_ref, bh_ref):
    by_a = (dot_t(by_ref[0], wg_ref[...]) + dot_t(by_ref[1], wu_ref[...])).astype(BF16).astype(F32)
    h = h_ref[...].astype(F32)
    scale = scale_of(h)
    by_h = scale * (by_a - h * (scale * scale * jnp.mean(by_a * h, -1, keepdims=True)))
    bh_ref[...] = (dy_ref[...].astype(F32) + by_h).astype(BF16)


def input_back(h, dy, by, wg, wu, layer, term, which, collective_id):
    t, d = h.shape
    ff = wg.shape[2]
    rows = lambda n: pl.BlockSpec((ROWS, n), lambda i: (i, 0))
    return scattering(
        input_back_kernel, t // ROWS, (0, 2),
        [rows(d), rows(d), pl.BlockSpec((2, ROWS, ff), lambda i: (0, i, 0)), whole(wg, layer), whole(wu, layer)],
        (h, dy, by, wg, wu),
        [rows(d)], [jax.ShapeDtypeStruct((t, d), BF16)],
        term, which, collective_id, "input_back", cost(4 * t * d * ff, 6 * t * ff),
    )


def hidden_back_kernel(by_ref, gate_ref, up_ref, wd_ref, out_ref):
    for start in range(0, gate_ref.shape[1], CHUNK):
        cols = pl.ds(start, CHUNK)
        by_act = dot_t(by_ref[...], wd_ref[cols, :]).astype(BF16).astype(F32)
        _, out_ref[0, :, cols], out_ref[1, :, cols] = gate_up_back(gate_ref[:, cols], up_ref[:, cols], by_act)


def hidden_back(by, gate, up, wd, layer, term, which, collective_id):
    t, d = by.shape
    ff = gate.shape[1]
    rows = lambda n: pl.BlockSpec((ROWS, n), lambda i: (i, 0))
    return scattering(
        hidden_back_kernel, t // ROWS, (0, 2),
        [rows(d), rows(ff), rows(ff), whole(wd, layer)], (by, gate, up, wd),
        [pl.BlockSpec((2, ROWS, ff), lambda i: (0, i, 0))], [jax.ShapeDtypeStruct((2, t, ff), BF16)],
        term, which, collective_id, "hidden_back", cost(2 * t * d * ff, 12 * t * ff),
    )


def product_kernel(a_ref, b_ref, c_ref):
    c_ref[...] = dot(a_ref[...], b_ref[...]).astype(BF16)


def product(a, b, name):
    (m, k), n = a.shape, b.shape[1]
    return pl.pallas_call(
        product_kernel,
        grid=(m // CHUNK,),
        in_specs=[pl.BlockSpec((CHUNK, k), lambda i: (i, 0)), pl.BlockSpec((k, n), lambda i: (0, 0), pipeline_mode=pl.Buffered(1))],
        out_specs=pl.BlockSpec((CHUNK, n), lambda i: (i, 0)),
        out_shape=jax.ShapeDtypeStruct((m, n), BF16),
        compiler_params=params(),
        cost_estimate=cost(2 * m * n * k, 2 * (m * k + k * n + m * n)),
        name=name,
    )(a, b)


def products(a, b, those, steps, term, which, collective_id):
    (m, k), n = a.shape, b.shape[2]
    chunks = n // CHUNK
    grid = len(those) * chunks
    first = those[0]
    return scattering(
        product_kernel, grid, steps,
        [pl.BlockSpec((m, k), lambda i: (0, 0), pipeline_mode=pl.Buffered(1)), pl.BlockSpec((None, k, CHUNK), lambda i: (first + i // chunks, 0, lax.rem(i, chunks)))],
        (a, b),
        [pl.BlockSpec((None, m, CHUNK), lambda i: (i // chunks, 0, lax.rem(i, chunks)))], [jax.ShapeDtypeStruct((len(those), m, n), BF16)],
        term, which, collective_id, "products", cost(2 * m * n * k * len(those), 2 * (m * k + k * n + m * n) * len(those)),
    )


def adamw_kernel(factor_ref, w_ref, m_ref, v_ref, g_ref, *refs):
    new_w_ref, new_m_ref, new_v_ref = refs[-3:]
    g = g_ref[...].astype(F32) * factor_ref[0, 0]
    m = 0.9 * m_ref[...] + 0.1 * g
    v = 0.95 * v_ref[...] + 0.05 * g * g
    w = w_ref[...].astype(F32)
    new_w_ref[...] = (w - 0.02 * (m * lax.rsqrt(v + 1e-8) + 0.1 * w)).astype(BF16)
    new_m_ref[...] = m
    new_v_ref[...] = v


def adamw(factor, w, m, v, g, layer, so_far):
    _, r, c = w.shape
    block = r // 7 if r % 112 == 0 else r // 8
    part = pl.BlockSpec((None, block, c), lambda i: (layer, i, 0))
    return pl.pallas_call(
        adamw_kernel,
        grid=(r // block,),
        in_specs=[pl.BlockSpec(memory_space=pltpu.SMEM), part, part, part, pl.BlockSpec((block, c), lambda i: (i, 0))]
        + [pl.BlockSpec(memory_space=pl.ANY)] * len(so_far),
        out_specs=[part] * 3,
        out_shape=[jax.ShapeDtypeStruct(w.shape, dtype) for dtype in (BF16, F32, F32)],
        input_output_aliases={5 + i: i for i in range(len(so_far))},
        compiler_params=params(),
        cost_estimate=cost(40 * r * c, 22 * r * c),
        name="adamw",
    )(factor, w, m, v, g, *so_far)


def solution(mesh):
    def step(x, dy, *arrays):
        weights, ms, vs = (arrays[i : i + 3] for i in (0, 3, 6))
        x, dy = x[0], dy[0]
        gather = lambda g: lax.all_gather(g, "dp", axis=0, tiled=True)

        at0, gate0, up0, actt0, h1 = forward(x, *weights, 0)
        at1, actt1, by1 = top(h1, dy, *weights, 1)
        shards, squares = [[None] * 3, [None] * 3], []

        def keep(layer, i, shard, square):
            shards[layer][i] = shard
            squares.append(square)

        down1 = product(actt1, dy, "down1")
        pair1, *rest = products(at1, by1, (0, 1), (0, 3), down1, None, 1)
        keep(1, 2, *rest)
        bh1, *rest = input_back(h1, dy, by1, *weights[:2], 1, pair1, 0, 2)
        keep(1, 0, *rest)
        down0 = product(actt0, bh1, "down0")
        by0, *rest = hidden_back(bh1, gate0, up0, weights[2], 0, pair1, 1, 3)
        keep(1, 1, *rest)
        gate_term, *rest = products(at0, by0, (0,), (0, 2), down0, None, 4)
        keep(0, 2, *rest)
        up_term, *rest = products(at0, by0, (1,), (0, 2), gate_term, 0, 5)
        keep(0, 0, *rest)
        keep(0, 1, *scattering(None, 1, (0, 0), [], (), [], [], up_term, 0, 6, "scatter", cost(2**30, 2**20)))
        total = lax.psum(sum(jnp.sum(square) for square in squares), "dp")
        count = sum(w.size for w in weights)
        factor = jnp.minimum(1.0, 0.5 * lax.rsqrt(total / count + 1e-30)).reshape(1, 1)

        new = [()] * 3
        for layer in (1, 0):
            for i in (2, 0, 1):
                new[i] = adamw(factor, weights[i], ms[i], vs[i], gather(shards[layer][i]), layer, new[i])
        return tuple(one[which] for which in range(3) for one in new)

    return jax.shard_map(
        step,
        mesh=mesh,
        in_specs=(P(("rep", "dp"), None, None),) * 2 + (P(None, None, None),) * 9,
        out_specs=(P("rep", None, None),) * 9,
        check_vma=False,
    )
```

```python
import jax
import jax.numpy as jnp
from jax import lax
from jax.experimental import pallas as pl
from jax.experimental.pallas import tpu as pltpu
from jax.sharding import PartitionSpec as P

BF16, F32 = jnp.bfloat16, jnp.float32
ROWS = 512
CHUNK = 768
VMEM_LIMIT = 62 * 1024 * 1024


def dot(a, b):
    return jnp.dot(a, b, preferred_element_type=F32)


def dot_t(a, b):
    return lax.dot_general(a, b, (((1,), (1,)), ((), ())), preferred_element_type=F32)


def scale_of(h):
    return lax.rsqrt(jnp.mean(h * h, -1, keepdims=True) + 1e-6)


def sigmoid(x):
    return 1.0 / (1.0 + jnp.exp(-x))


def params(n=1):
    return pltpu.CompilerParams(dimension_semantics=("arbitrary",) * n, vmem_limit_bytes=VMEM_LIMIT)


def cost(flops, nbytes):
    return pl.CostEstimate(flops=flops, bytes_accessed=nbytes, transcendentals=0)


def whole(w, layer):
    return pl.BlockSpec((None,) + w.shape[1:], lambda *_: (layer, 0, 0), pipeline_mode=pl.Buffered(1))


def forward_kernel(h_ref, wg_ref, wu_ref, wd_ref, at_ref, gate_ref, up_ref, actt_ref, y_ref):
    h = h_ref[...].astype(F32)
    a = (h * scale_of(h)).astype(BF16)
    at_ref[...] = a.T
    acts = []
    for start in range(0, wg_ref.shape[1], CHUNK):
        cols = pl.ds(start, CHUNK)
        gate, up = dot(a, wg_ref[:, cols]), dot(a, wu_ref[:, cols])
        gate_ref[:, cols] = gate
        up_ref[:, cols] = up
        act = (gate * sigmoid(gate) * up).astype(BF16)
        actt_ref[cols, :] = act.T
        acts.append(act)
    y = dot(jnp.concatenate(acts, 1), wd_ref[...]).astype(BF16)
    y_ref[...] = h_ref[...] + y


def forward(h, wg, wu, wd, layer):
    t, d = h.shape
    ff = wg.shape[2]
    rows = lambda n: pl.BlockSpec((ROWS, n), lambda i: (i, 0))
    cols = lambda n: pl.BlockSpec((n, ROWS), lambda i: (0, i))
    return pl.pallas_call(
        forward_kernel,
        grid=(t // ROWS,),
        in_specs=[rows(d), whole(wg, layer), whole(wu, layer), whole(wd, layer)],
        out_specs=[cols(d), rows(ff), rows(ff), cols(ff), rows(d)],
        out_shape=[
            jax.ShapeDtypeStruct((d, t), BF16),
            jax.ShapeDtypeStruct((t, ff), F32),
            jax.ShapeDtypeStruct((t, ff), F32),
            jax.ShapeDtypeStruct((ff, t), BF16),
            jax.ShapeDtypeStruct((t, d), BF16),
        ],
        compiler_params=params(),
        cost_estimate=cost(6 * t * d * ff, 12 * t * ff),
        name="forward",
    )(h, wg, wu, wd)


def gate_up_back(gate, up, by_act):
    sig = sigmoid(gate)
    silu = gate * sig
    by_gate = by_act * up * (sig + silu * (1.0 - sig))
    return (silu * up).astype(BF16), by_gate.astype(BF16), (by_act * silu).astype(BF16)


def top_kernel(h_ref, dy_ref, wg_ref, wu_ref, wd_ref, at_ref, actt_ref, by_ref):
    h = h_ref[...].astype(F32)
    a = (h * scale_of(h)).astype(BF16)
    at_ref[...] = a.T
    for start in range(0, wg_ref.shape[1], CHUNK):
        cols = pl.ds(start, CHUNK)
        by_act = dot_t(dy_ref[...], wd_ref[cols, :]).astype(BF16).astype(F32)
        act, by_ref[0, :, cols], by_ref[1, :, cols] = gate_up_back(dot(a, wg_ref[:, cols]), dot(a, wu_ref[:, cols]), by_act)
        actt_ref[cols, :] = act.T


def top(h, dy, wg, wu, wd, layer):
    t, d = h.shape
    ff = wg.shape[2]
    rows = lambda n: pl.BlockSpec((ROWS, n), lambda i: (i, 0))
    cols = lambda n: pl.BlockSpec((n, ROWS), lambda i: (0, i))
    return pl.pallas_call(
        top_kernel,
        grid=(t // ROWS,),
        in_specs=[rows(d), rows(d), whole(wg, layer), whole(wu, layer), whole(wd, layer)],
        out_specs=[cols(d), cols(ff), pl.BlockSpec((2, ROWS, ff), lambda i: (0, i, 0))],
        out_shape=[
            jax.ShapeDtypeStruct((d, t), BF16),
            jax.ShapeDtypeStruct((ff, t), BF16),
            jax.ShapeDtypeStruct((2, t, ff), BF16),
        ],
        compiler_params=params(),
        cost_estimate=cost(6 * t * d * ff, 8 * t * ff),
        name="top",
    )(h, dy, wg, wu, wd)


class Scatter:
    def __init__(self, g, out, squares, mine, got1, send2, got2, send3, got3, local, sent, received):
        self.g, self.out, self.squares = g, out, squares
        self.mine, self.got1, self.send2, self.got2, self.send3, self.got3 = mine, got1, send2, got2, send3, got3
        self.local, self.sent, self.received = local, sent, received
        me = lax.axis_index("dp")
        self.x, self.y, self.core = me // 4, lax.rem(me // 2, 2), lax.rem(me, 2)
        self.over_core, self.over_x, self.over_y = (self.device(*flip) for flip in ((0, 0, 1), (1, 0, 0), (0, 1, 0)))

    def device(self, x, y, core):
        flip = lambda at, by: 1 - at if by else at
        return {"dp": flip(self.x, x) * 4 + flip(self.y, y) * 2 + flip(self.core, core)}

    def part(self, ref, at, half):
        r, c = half_shape(*ref.shape[1:])
        if r == ref.shape[1]:
            return ref[at, :, half * c : (half + 1) * c]
        return ref[at, half * r : (half + 1) * r, :]

    def own(self, at, half):
        return self.part(self.mine, at, half).astype(F32) + self.part(self.got1, at, half).astype(F32)

    def send(self, src, dst, number, device):
        return pltpu.make_async_remote_copy(
            src_ref=src, dst_ref=dst, send_sem=self.sent.at[number], recv_sem=self.received.at[number],
            device_id=device, device_id_type=pl.DeviceIdType.MESH,
        )

    def fetch(self):
        return pltpu.make_async_copy(self.g.at[:, self.core], self.mine, self.local)

    def first(self):
        return self.send(self.g.at[:, 1 - self.core], self.got1, 0, self.over_core)

    def pair(self, src, dst, number, devices):
        return [self.send(src.at[half], dst.at[half], number + half, devices[half]) for half in range(2)]

    def second(self):
        return self.pair(self.send2, self.got2, 1, (self.over_x, self.over_y))

    def third(self):
        return self.pair(self.send3, self.got3, 3, (self.over_y, self.over_x))

    def begin(self):
        barrier = pltpu.get_barrier_semaphore()
        for device in (self.over_core, self.over_x, self.over_y):
            pl.semaphore_signal(barrier, inc=1, device_id=device, device_id_type=pl.DeviceIdType.MESH)
        pl.semaphore_wait(barrier, 3)
        self.first().start()
        self.fetch().start()

    def go_second(self):
        self.fetch().wait()
        self.first().wait()
        for j in range(2):
            self.send2[0, j] = self.own(2 * (1 - self.x) + j, 0).astype(BF16)
            self.send2[1, j] = self.own(2 * j + (1 - self.y), 1).astype(BF16)
        for copy in self.second():
            copy.start()

    def go_third(self):
        for copy in self.second():
            copy.wait()
        x, y = self.x, self.y
        self.send3[0] = (self.own(2 * x + (1 - y), 0) + self.got2[0, 1 - y].astype(F32)).astype(BF16)
        self.send3[1] = (self.own(2 * (1 - x) + y, 1) + self.got2[1, 1 - x].astype(F32)).astype(BF16)
        for copy in self.third():
            copy.start()

    def end(self):
        for copy in self.third():
            copy.wait()
        x, y = self.x, self.y
        r, c = self.out.shape
        hr, hc = half_shape(r, c)
        for half, kept in ((0, self.got2[0, y]), (1, self.got2[1, x])):
            total = (self.own(2 * x + y, half) + kept.astype(F32) + self.got3[half].astype(F32)).astype(BF16)
            square = jnp.square(total.astype(F32))
            if hr == r:
                self.out[:, half * hc : (half + 1) * hc] = total
                self.squares[:, half * hc : (half + 1) * hc] = jnp.sum(square, 0, keepdims=True)
            else:
                self.out[half * hr : (half + 1) * hr, :] = total
                square = jnp.sum(square, 0, keepdims=True)
                self.squares[...] = square if half == 0 else self.squares[...] + square


def half_shape(r, c):
    return (r, c // 2) if c % 256 == 0 else (r // 2, c)


def scatter_scratch(r, c):
    hr, hc = half_shape(r, c)
    blocks = ((4, r, c), (4, r, c), (2, 2, hr, hc), (2, 2, hr, hc), (2, hr, hc), (2, hr, hc))
    return [pltpu.VMEM(block, BF16) for block in blocks] + [pltpu.SemaphoreType.DMA, pltpu.SemaphoreType.DMA((5,)), pltpu.SemaphoreType.DMA((5,))]


def by_device(term):
    r, c = term.shape[-2:]
    return term.reshape(term.shape[:-2] + (4, 2, r // 8, c))


def scattering(compute, grid, steps, in_specs, args, out_specs, out_shape, term, which, collective_id, name, cost_estimate):
    term = by_device(term)
    r, c = term.shape[-2:]
    n_in, n_out = len(args), len(out_shape)

    def kernel(*refs):
        ins, g, outs, (out, squares), scratch = refs[:n_in], refs[n_in], refs[n_in + 1 :][:n_out], refs[n_in + 1 + n_out :][:2], refs[n_in + 3 + n_out :]
        scatter = Scatter(g if which is None else g.at[which], out, squares, *scratch)
        step = pl.program_id(0)
        pl.when(step == 0)(scatter.begin)
        compute(*ins, *outs)
        pl.when(step == steps[0])(scatter.go_second)
        pl.when(step == steps[1])(scatter.go_third)
        pl.when(step == grid - 1)(scatter.end)

    fixed = lambda *shape: pl.BlockSpec(shape, lambda i: (0,) * len(shape))
    return pl.pallas_call(
        kernel,
        grid=(grid,),
        in_specs=list(in_specs) + [pl.BlockSpec(memory_space=pl.ANY)],
        out_specs=list(out_specs) + [fixed(r, c), fixed(1, c)],
        out_shape=list(out_shape) + [jax.ShapeDtypeStruct((r, c), BF16), jax.ShapeDtypeStruct((1, c), F32)],
        scratch_shapes=scatter_scratch(r, c),
        compiler_params=pltpu.CompilerParams(
            dimension_semantics=("arbitrary",), vmem_limit_bytes=VMEM_LIMIT, collective_id=collective_id, has_side_effects=True
        ),
        cost_estimate=cost_estimate,
        name=name,
    )(*args, term)


def last_scatter(term, which, squares, collective_id):
    term = by_device(term)
    r, c = term.shape[-2:]

    def kernel(*refs):
        g, others, (out, total_ref), (own, mine, theirs, *scratch) = refs[0], refs[1 : 1 + len(squares)], refs[1 + len(squares) :][:2], refs[3 + len(squares) :]
        *scratch, sent, received = scratch
        scatter = Scatter(g.at[which], out, own, *scratch)
        scatter.begin()
        rest = sum(jnp.sum(other[...], keepdims=True) for other in others)
        scatter.go_second()
        scatter.go_third()
        scatter.end()
        total = jnp.broadcast_to(rest + jnp.sum(own[...], keepdims=True), (8, 128))
        for i, device in enumerate((scatter.over_core, scatter.over_x, scatter.over_y)):
            mine[i] = total
            copy = pltpu.make_async_remote_copy(
                src_ref=mine.at[i], dst_ref=theirs.at[i], send_sem=sent.at[i], recv_sem=received.at[i],
                device_id=device, device_id_type=pl.DeviceIdType.MESH,
            )
            copy.start()
            copy.wait()
            total = total + theirs[i]
        total_ref[...] = total

    vmem = pl.BlockSpec(memory_space=pltpu.VMEM)
    return pl.pallas_call(
        kernel,
        in_specs=[pl.BlockSpec(memory_space=pl.ANY)] + [vmem] * len(squares),
        out_specs=[vmem, vmem],
        out_shape=[jax.ShapeDtypeStruct((r, c), BF16), jax.ShapeDtypeStruct((8, 128), F32)],
        scratch_shapes=[pltpu.VMEM((1, c), F32), pltpu.VMEM((3, 8, 128), F32), pltpu.VMEM((3, 8, 128), F32)]
        + scatter_scratch(r, c)
        + [pltpu.SemaphoreType.DMA((3,)), pltpu.SemaphoreType.DMA((3,))],
        compiler_params=pltpu.CompilerParams(vmem_limit_bytes=VMEM_LIMIT, collective_id=collective_id, has_side_effects=True),
        cost_estimate=cost(2**34, 2**20),
        name="last_scatter",
    )(term, *squares)


def input_back_kernel(h_ref, dy_ref, by_ref, wg_ref, wu_ref, bh_ref):
    by_a = (dot_t(by_ref[0], wg_ref[...]) + dot_t(by_ref[1], wu_ref[...])).astype(BF16).astype(F32)
    h = h_ref[...].astype(F32)
    scale = scale_of(h)
    by_h = scale * (by_a - h * (scale * scale * jnp.mean(by_a * h, -1, keepdims=True)))
    bh_ref[...] = (dy_ref[...].astype(F32) + by_h).astype(BF16)


def input_back(h, dy, by, wg, wu, layer, term, which, collective_id):
    t, d = h.shape
    ff = wg.shape[2]
    rows = lambda n: pl.BlockSpec((ROWS, n), lambda i: (i, 0))
    return scattering(
        input_back_kernel, t // ROWS, (0, 2),
        [rows(d), rows(d), pl.BlockSpec((2, ROWS, ff), lambda i: (0, i, 0)), whole(wg, layer), whole(wu, layer)],
        (h, dy, by, wg, wu),
        [rows(d)], [jax.ShapeDtypeStruct((t, d), BF16)],
        term, which, collective_id, "input_back", cost(4 * t * d * ff, 6 * t * ff),
    )


def hidden_back_kernel(by_ref, gate_ref, up_ref, wd_ref, out_ref):
    for start in range(0, gate_ref.shape[1], CHUNK):
        cols = pl.ds(start, CHUNK)
        by_act = dot_t(by_ref[...], wd_ref[cols, :]).astype(BF16).astype(F32)
        _, out_ref[0, :, cols], out_ref[1, :, cols] = gate_up_back(gate_ref[:, cols], up_ref[:, cols], by_act)


def hidden_back(by, gate, up, wd, layer, term, which, collective_id):
    t, d = by.shape
    ff = gate.shape[1]
    rows = lambda n: pl.BlockSpec((ROWS, n), lambda i: (i, 0))
    return scattering(
        hidden_back_kernel, t // ROWS, (0, 2),
        [rows(d), rows(ff), rows(ff), whole(wd, layer)], (by, gate, up, wd),
        [pl.BlockSpec((2, ROWS, ff), lambda i: (0, i, 0))], [jax.ShapeDtypeStruct((2, t, ff), BF16)],
        term, which, collective_id, "hidden_back", cost(2 * t * d * ff, 12 * t * ff),
    )


def product_kernel(a_ref, b_ref, c_ref):
    c_ref[...] = dot(a_ref[...], b_ref[...]).astype(BF16)


def product(a, b, name):
    (m, k), n = a.shape, b.shape[1]
    return pl.pallas_call(
        product_kernel,
        grid=(m // CHUNK,),
        in_specs=[pl.BlockSpec((CHUNK, k), lambda i: (i, 0)), pl.BlockSpec((k, n), lambda i: (0, 0), pipeline_mode=pl.Buffered(1))],
        out_specs=pl.BlockSpec((CHUNK, n), lambda i: (i, 0)),
        out_shape=jax.ShapeDtypeStruct((m, n), BF16),
        compiler_params=params(),
        cost_estimate=cost(2 * m * n * k, 2 * (m * k + k * n + m * n)),
        name=name,
    )(a, b)


def products(a, b, those, steps, term, which, collective_id):
    (m, k), n = a.shape, b.shape[2]
    chunks = n // CHUNK
    grid = len(those) * chunks
    first = those[0]
    return scattering(
        product_kernel, grid, steps,
        [pl.BlockSpec((m, k), lambda i: (0, 0), pipeline_mode=pl.Buffered(1)), pl.BlockSpec((None, k, CHUNK), lambda i: (first + i // chunks, 0, lax.rem(i, chunks)))],
        (a, b),
        [pl.BlockSpec((None, m, CHUNK), lambda i: (i // chunks, 0, lax.rem(i, chunks)))], [jax.ShapeDtypeStruct((len(those), m, n), BF16)],
        term, which, collective_id, "products", cost(2 * m * n * k * len(those), 2 * (m * k + k * n + m * n) * len(those)),
    )


def adamw(total, count, items, layer):
    blocks = [w.shape[1] // 7 if w.shape[1] % 112 == 0 else w.shape[1] // 8 for w, *_ in items]
    steps = [w.shape[1] // block for (w, *_), block in zip(items, blocks, strict=True)]
    starts = [sum(steps[:i]) for i in range(len(items))]
    n_far = sum(len(so_far) for *_, so_far in items)

    def kernel(total_ref, *refs):
        factor = jnp.minimum(1.0, 0.5 * lax.rsqrt(total_ref[0:1, 0:1] / count + 1e-30))
        ins, outs = refs[: 4 * len(items)], refs[4 * len(items) + n_far :]
        for i in range(len(items)):
            w_ref, m_ref, v_ref, g_ref = ins[4 * i : 4 * i + 4]
            new_w_ref, new_m_ref, new_v_ref = outs[3 * i : 3 * i + 3]

            def update(w_ref=w_ref, m_ref=m_ref, v_ref=v_ref, g_ref=g_ref, new_w_ref=new_w_ref, new_m_ref=new_m_ref, new_v_ref=new_v_ref):
                g = g_ref[...].astype(F32) * factor
                m = 0.9 * m_ref[...] + 0.1 * g
                v = 0.95 * v_ref[...] + 0.05 * g * g
                w = w_ref[...].astype(F32)
                new_w_ref[...] = (w - 0.02 * (m * lax.rsqrt(v + 1e-8) + 0.1 * w)).astype(BF16)
                new_m_ref[...] = m
                new_v_ref[...] = v

            if len(items) == 1:
                update()
            else:
                step = pl.program_id(0)
                pl.when((step >= starts[i]) & (step < starts[i] + steps[i]))(update)

    in_specs, args, out_specs, out_shape = [pl.BlockSpec((8, 128), lambda i: (0, 0))], [total], [], []
    for (w, m, v, g, _), block, n, start in zip(items, blocks, steps, starts, strict=True):
        at = lambda i, n=n, start=start: jnp.clip(i - start, 0, n - 1)
        part = pl.BlockSpec((None, block, w.shape[2]), lambda i, at=at: (layer, at(i), 0))
        in_specs += [part, part, part, pl.BlockSpec((block, w.shape[2]), lambda i, at=at: (at(i), 0))]
        args += [w, m, v, g]
        out_specs += [part] * 3
        out_shape += [jax.ShapeDtypeStruct(w.shape, dtype) for dtype in (BF16, F32, F32)]
    far = [one for *_, so_far in items for one in so_far]
    size = sum(w.size for w, *_ in items) // 2
    new = pl.pallas_call(
        kernel,
        grid=(sum(steps),),
        in_specs=in_specs + [pl.BlockSpec(memory_space=pl.ANY)] * n_far,
        out_specs=out_specs,
        out_shape=out_shape,
        input_output_aliases={len(args) + i: i for i in range(n_far)},
        compiler_params=params(),
        cost_estimate=cost(40 * size, 22 * size),
        name="adamw",
    )(*args, *far)
    return [tuple(new[3 * i : 3 * i + 3]) for i in range(len(items))]


def solution(mesh):
    def step(x, dy, *arrays):
        weights, ms, vs = (arrays[i : i + 3] for i in (0, 3, 6))
        x, dy = x[0], dy[0]
        gather = lambda g: lax.all_gather(g, "dp", axis=0, tiled=True)

        at0, gate0, up0, actt0, h1 = forward(x, *weights, 0)
        at1, actt1, by1 = top(h1, dy, *weights, 1)
        shards, squares = [[None] * 3, [None] * 3], []

        def keep(layer, i, shard, square):
            shards[layer][i] = shard
            squares.append(square)

        down1 = product(actt1, dy, "down1")
        pair1, *rest = products(at1, by1, (0, 1), (0, 3), down1, None, 1)
        keep(1, 2, *rest)
        bh1, *rest = input_back(h1, dy, by1, *weights[:2], 1, pair1, 0, 2)
        keep(1, 0, *rest)
        down0 = product(actt0, bh1, "down0")
        by0, *rest = hidden_back(bh1, gate0, up0, weights[2], 0, pair1, 1, 3)
        keep(1, 1, *rest)
        gate_term, *rest = products(at0, by0, (0,), (0, 2), down0, None, 4)
        keep(0, 2, *rest)
        up_term, *rest = products(at0, by0, (1,), (0, 2), gate_term, 0, 5)
        keep(0, 0, *rest)
        shards[0][1], total = last_scatter(up_term, 0, squares, 6)
        held, _ = lax.optimization_barrier((shards[0], total))

        count = sum(w.size for w in weights)
        order = (2, 0, 1)
        items = [(weights[i], ms[i], vs[i], gather(shards[1][i]), ()) for i in order]
        new = dict(zip(order, adamw(total, count, items, 1), strict=True))
        for i in order:
            (new[i],) = adamw(total, count, [(weights[i], ms[i], vs[i], gather(held[i]), new[i])], 0)
        new = [new[i] for i in range(3)]
        return tuple(one[which] for which in range(3) for one in new)

    return jax.shard_map(
        step,
        mesh=mesh,
        in_specs=(P(("rep", "dp"), None, None),) * 2 + (P(None, None, None),) * 9,
        out_specs=(P("rep", None, None),) * 9,
        check_vma=False,
    )
```

```python
import jax
import jax.numpy as jnp
from jax import lax
from jax.experimental import pallas as pl
from jax.experimental.pallas import tpu as pltpu
from jax.sharding import PartitionSpec as P

BF16, F32 = jnp.bfloat16, jnp.float32
ROWS = 512
CHUNK = 768
VMEM_LIMIT = 62 * 1024 * 1024


def dot(a, b):
    return jnp.dot(a, b, preferred_element_type=F32)


def dot_t(a, b):
    return lax.dot_general(a, b, (((1,), (1,)), ((), ())), preferred_element_type=F32)


def scale_of(h):
    return lax.rsqrt(jnp.mean(h * h, -1, keepdims=True) + 1e-6)


def sigmoid(x):
    return 1.0 / (1.0 + jnp.exp(-x))


def params(n=1):
    return pltpu.CompilerParams(dimension_semantics=("arbitrary",) * n, vmem_limit_bytes=VMEM_LIMIT)


def cost(flops, nbytes):
    return pl.CostEstimate(flops=flops, bytes_accessed=nbytes, transcendentals=0)


def whole(w, layer):
    return pl.BlockSpec((None,) + w.shape[1:], lambda *_: (layer, 0, 0), pipeline_mode=pl.Buffered(1))


def forward_kernel(h_ref, wg_ref, wu_ref, wd_ref, at_ref, gate_ref, up_ref, actt_ref, y_ref):
    h = h_ref[...].astype(F32)
    a = (h * scale_of(h)).astype(BF16)
    at_ref[...] = a.T
    acts = []
    for start in range(0, wg_ref.shape[1], CHUNK):
        cols = pl.ds(start, CHUNK)
        gate, up = dot(a, wg_ref[:, cols]), dot(a, wu_ref[:, cols])
        gate_ref[:, cols] = gate
        up_ref[:, cols] = up
        act = (gate * sigmoid(gate) * up).astype(BF16)
        actt_ref[cols, :] = act.T
        acts.append(act)
    y = dot(jnp.concatenate(acts, 1), wd_ref[...]).astype(BF16)
    y_ref[...] = h_ref[...] + y


def forward(h, wg, wu, wd, layer):
    t, d = h.shape
    ff = wg.shape[2]
    rows = lambda n: pl.BlockSpec((ROWS, n), lambda i: (i, 0))
    cols = lambda n: pl.BlockSpec((n, ROWS), lambda i: (0, i))
    return pl.pallas_call(
        forward_kernel,
        grid=(t // ROWS,),
        in_specs=[rows(d), whole(wg, layer), whole(wu, layer), whole(wd, layer)],
        out_specs=[cols(d), rows(ff), rows(ff), cols(ff), rows(d)],
        out_shape=[
            jax.ShapeDtypeStruct((d, t), BF16),
            jax.ShapeDtypeStruct((t, ff), F32),
            jax.ShapeDtypeStruct((t, ff), F32),
            jax.ShapeDtypeStruct((ff, t), BF16),
            jax.ShapeDtypeStruct((t, d), BF16),
        ],
        compiler_params=params(),
        cost_estimate=cost(6 * t * d * ff, 12 * t * ff),
        name="forward",
    )(h, wg, wu, wd)


def gate_up_back(gate, up, by_act):
    sig = sigmoid(gate)
    silu = gate * sig
    by_gate = by_act * up * (sig + silu * (1.0 - sig))
    return (silu * up).astype(BF16), by_gate.astype(BF16), (by_act * silu).astype(BF16)


def top_kernel(h_ref, dy_ref, wg_ref, wu_ref, wd_ref, at_ref, actt_ref, by_ref):
    h = h_ref[...].astype(F32)
    a = (h * scale_of(h)).astype(BF16)
    at_ref[...] = a.T
    for start in range(0, wg_ref.shape[1], CHUNK):
        cols = pl.ds(start, CHUNK)
        by_act = dot_t(dy_ref[...], wd_ref[cols, :]).astype(BF16).astype(F32)
        act, by_ref[0, :, cols], by_ref[1, :, cols] = gate_up_back(dot(a, wg_ref[:, cols]), dot(a, wu_ref[:, cols]), by_act)
        actt_ref[cols, :] = act.T


def top(h, dy, wg, wu, wd, layer):
    t, d = h.shape
    ff = wg.shape[2]
    rows = lambda n: pl.BlockSpec((ROWS, n), lambda i: (i, 0))
    cols = lambda n: pl.BlockSpec((n, ROWS), lambda i: (0, i))
    return pl.pallas_call(
        top_kernel,
        grid=(t // ROWS,),
        in_specs=[rows(d), rows(d), whole(wg, layer), whole(wu, layer), whole(wd, layer)],
        out_specs=[cols(d), cols(ff), pl.BlockSpec((2, ROWS, ff), lambda i: (0, i, 0))],
        out_shape=[
            jax.ShapeDtypeStruct((d, t), BF16),
            jax.ShapeDtypeStruct((ff, t), BF16),
            jax.ShapeDtypeStruct((2, t, ff), BF16),
        ],
        compiler_params=params(),
        cost_estimate=cost(6 * t * d * ff, 8 * t * ff),
        name="top",
    )(h, dy, wg, wu, wd)


class Scatter:
    def __init__(self, g, out, squares, mine, got1, send2, got2, send3, got3, local, sent, received):
        self.g, self.out, self.squares = g, out, squares
        self.mine, self.got1, self.send2, self.got2, self.send3, self.got3 = mine, got1, send2, got2, send3, got3
        self.local, self.sent, self.received = local, sent, received
        me = lax.axis_index("dp")
        self.x, self.y, self.core = me // 4, lax.rem(me // 2, 2), lax.rem(me, 2)
        self.over_core, self.over_x, self.over_y = (self.device(*flip) for flip in ((0, 0, 1), (1, 0, 0), (0, 1, 0)))

    def device(self, x, y, core):
        flip = lambda at, by: 1 - at if by else at
        return {"dp": flip(self.x, x) * 4 + flip(self.y, y) * 2 + flip(self.core, core)}

    def part(self, ref, at, half):
        r, c = half_shape(*ref.shape[1:])
        if r == ref.shape[1]:
            return ref[at, :, half * c : (half + 1) * c]
        return ref[at, half * r : (half + 1) * r, :]

    def own(self, at, half):
        return self.part(self.mine, at, half).astype(F32) + self.part(self.got1, at, half).astype(F32)

    def send(self, src, dst, number, device):
        return pltpu.make_async_remote_copy(
            src_ref=src, dst_ref=dst, send_sem=self.sent.at[number], recv_sem=self.received.at[number],
            device_id=device, device_id_type=pl.DeviceIdType.MESH,
        )

    def fetch(self):
        return pltpu.make_async_copy(self.g.at[:, self.core], self.mine, self.local)

    def first(self):
        r, c = half_shape(*self.got1.shape[1:])
        whole_rows = r == self.got1.shape[1]
        copies = []
        for at in range(4):
            for half in range(2):
                rows, cols = (pl.ds(0, r), pl.ds(half * c, c)) if whole_rows else (pl.ds(half * r, r), pl.ds(0, c))
                copies.append(self.send(self.g.at[at, 1 - self.core, rows, cols], self.got1.at[at, rows, cols], 4 + len(copies), self.over_core))
        return copies

    def pair(self, src, dst, number, devices):
        return [self.send(src.at[half], dst.at[half], number + half, devices[half]) for half in range(2)]

    def second(self):
        return self.pair(self.send2, self.got2, 0, (self.over_x, self.over_y))

    def third(self):
        return self.pair(self.send3, self.got3, 2, (self.over_y, self.over_x))

    def begin(self):
        barrier = pltpu.get_barrier_semaphore()
        for device in (self.over_core, self.over_x, self.over_y):
            pl.semaphore_signal(barrier, inc=1, device_id=device, device_id_type=pl.DeviceIdType.MESH)
        pl.semaphore_wait(barrier, 3)
        for copy in self.first():
            copy.start()
        self.fetch().start()

    def go_second(self):
        self.fetch().wait()
        for copy in self.first():
            copy.wait()
        for j in range(2):
            self.send2[0, j] = self.own(2 * (1 - self.x) + j, 0).astype(BF16)
            self.send2[1, j] = self.own(2 * j + (1 - self.y), 1).astype(BF16)
        for copy in self.second():
            copy.start()

    def go_third(self):
        for copy in self.second():
            copy.wait()
        x, y = self.x, self.y
        self.send3[0] = (self.own(2 * x + (1 - y), 0) + self.got2[0, 1 - y].astype(F32)).astype(BF16)
        self.send3[1] = (self.own(2 * (1 - x) + y, 1) + self.got2[1, 1 - x].astype(F32)).astype(BF16)
        for copy in self.third():
            copy.start()

    def end(self):
        for copy in self.third():
            copy.wait()
        x, y = self.x, self.y
        r, c = self.out.shape
        hr, hc = half_shape(r, c)
        for half, kept in ((0, self.got2[0, y]), (1, self.got2[1, x])):
            total = (self.own(2 * x + y, half) + kept.astype(F32) + self.got3[half].astype(F32)).astype(BF16)
            square = jnp.square(total.astype(F32))
            if hr == r:
                self.out[:, half * hc : (half + 1) * hc] = total
                self.squares[:, half * hc : (half + 1) * hc] = jnp.sum(square, 0, keepdims=True)
            else:
                self.out[half * hr : (half + 1) * hr, :] = total
                square = jnp.sum(square, 0, keepdims=True)
                self.squares[...] = square if half == 0 else self.squares[...] + square


def half_shape(r, c):
    return (r, c // 2) if c % 256 == 0 else (r // 2, c)


def scatter_scratch(r, c):
    hr, hc = half_shape(r, c)
    blocks = ((4, r, c), (4, r, c), (2, 2, hr, hc), (2, 2, hr, hc), (2, hr, hc), (2, hr, hc))
    return [pltpu.VMEM(block, BF16) for block in blocks] + [pltpu.SemaphoreType.DMA, pltpu.SemaphoreType.DMA((12,)), pltpu.SemaphoreType.DMA((12,))]


def by_device(term):
    r, c = term.shape[-2:]
    return term.reshape(term.shape[:-2] + (4, 2, r // 8, c))


def scattering(compute, grid, steps, in_specs, args, out_specs, out_shape, term, which, collective_id, name, cost_estimate):
    term = by_device(term)
    r, c = term.shape[-2:]
    n_in, n_out = len(args), len(out_shape)

    def kernel(*refs):
        ins, g, outs, (out, squares), scratch = refs[:n_in], refs[n_in], refs[n_in + 1 :][:n_out], refs[n_in + 1 + n_out :][:2], refs[n_in + 3 + n_out :]
        scatter = Scatter(g if which is None else g.at[which], out, squares, *scratch)
        step = pl.program_id(0)
        pl.when(step == 0)(scatter.begin)
        compute(*ins, *outs)
        pl.when(step == steps[0])(scatter.go_second)
        pl.when(step == steps[1])(scatter.go_third)
        pl.when(step == grid - 1)(scatter.end)

    fixed = lambda *shape: pl.BlockSpec(shape, lambda i: (0,) * len(shape))
    return pl.pallas_call(
        kernel,
        grid=(grid,),
        in_specs=list(in_specs) + [pl.BlockSpec(memory_space=pl.ANY)],
        out_specs=list(out_specs) + [fixed(r, c), fixed(1, c)],
        out_shape=list(out_shape) + [jax.ShapeDtypeStruct((r, c), BF16), jax.ShapeDtypeStruct((1, c), F32)],
        scratch_shapes=scatter_scratch(r, c),
        compiler_params=pltpu.CompilerParams(
            dimension_semantics=("arbitrary",), vmem_limit_bytes=VMEM_LIMIT, collective_id=collective_id, has_side_effects=True
        ),
        cost_estimate=cost_estimate,
        name=name,
    )(*args, term)


def last_scatter(term, which, squares, collective_id):
    term = by_device(term)
    r, c = term.shape[-2:]

    def kernel(*refs):
        g, others, (out, total_ref), (own, mine, theirs, *scratch) = refs[0], refs[1 : 1 + len(squares)], refs[1 + len(squares) :][:2], refs[3 + len(squares) :]
        *scratch, sent, received = scratch
        scatter = Scatter(g.at[which], out, own, *scratch)
        scatter.begin()
        rest = sum(jnp.sum(other[...], keepdims=True) for other in others)
        scatter.go_second()
        scatter.go_third()
        scatter.end()
        total = jnp.broadcast_to(rest + jnp.sum(own[...], keepdims=True), (8, 128))
        for i, device in enumerate((scatter.over_core, scatter.over_x, scatter.over_y)):
            mine[i] = total
            copy = pltpu.make_async_remote_copy(
                src_ref=mine.at[i], dst_ref=theirs.at[i], send_sem=sent.at[i], recv_sem=received.at[i],
                device_id=device, device_id_type=pl.DeviceIdType.MESH,
            )
            copy.start()
            copy.wait()
            total = total + theirs[i]
        total_ref[...] = total

    vmem = pl.BlockSpec(memory_space=pltpu.VMEM)
    return pl.pallas_call(
        kernel,
        in_specs=[pl.BlockSpec(memory_space=pl.ANY)] + [vmem] * len(squares),
        out_specs=[vmem, vmem],
        out_shape=[jax.ShapeDtypeStruct((r, c), BF16), jax.ShapeDtypeStruct((8, 128), F32)],
        scratch_shapes=[pltpu.VMEM((1, c), F32), pltpu.VMEM((3, 8, 128), F32), pltpu.VMEM((3, 8, 128), F32)]
        + scatter_scratch(r, c)
        + [pltpu.SemaphoreType.DMA((3,)), pltpu.SemaphoreType.DMA((3,))],
        compiler_params=pltpu.CompilerParams(vmem_limit_bytes=VMEM_LIMIT, collective_id=collective_id, has_side_effects=True),
        cost_estimate=cost(2**34, 2**20),
        name="last_scatter",
    )(term, *squares)


def input_back_kernel(h_ref, dy_ref, by_ref, wg_ref, wu_ref, bh_ref):
    by_a = (dot_t(by_ref[0], wg_ref[...]) + dot_t(by_ref[1], wu_ref[...])).astype(BF16).astype(F32)
    h = h_ref[...].astype(F32)
    scale = scale_of(h)
    by_h = scale * (by_a - h * (scale * scale * jnp.mean(by_a * h, -1, keepdims=True)))
    bh_ref[...] = (dy_ref[...].astype(F32) + by_h).astype(BF16)


def input_back(h, dy, by, wg, wu, layer, term, which, collective_id):
    t, d = h.shape
    ff = wg.shape[2]
    rows = lambda n: pl.BlockSpec((ROWS, n), lambda i: (i, 0))
    return scattering(
        input_back_kernel, t // ROWS, (0, 2),
        [rows(d), rows(d), pl.BlockSpec((2, ROWS, ff), lambda i: (0, i, 0)), whole(wg, layer), whole(wu, layer)],
        (h, dy, by, wg, wu),
        [rows(d)], [jax.ShapeDtypeStruct((t, d), BF16)],
        term, which, collective_id, "input_back", cost(4 * t * d * ff, 6 * t * ff),
    )


def hidden_back_kernel(by_ref, gate_ref, up_ref, wd_ref, out_ref):
    for start in range(0, gate_ref.shape[1], CHUNK):
        cols = pl.ds(start, CHUNK)
        by_act = dot_t(by_ref[...], wd_ref[cols, :]).astype(BF16).astype(F32)
        _, out_ref[0, :, cols], out_ref[1, :, cols] = gate_up_back(gate_ref[:, cols], up_ref[:, cols], by_act)


def hidden_back(by, gate, up, wd, layer, term, which, collective_id):
    t, d = by.shape
    ff = gate.shape[1]
    rows = lambda n: pl.BlockSpec((ROWS, n), lambda i: (i, 0))
    return scattering(
        hidden_back_kernel, t // ROWS, (0, 2),
        [rows(d), rows(ff), rows(ff), whole(wd, layer)], (by, gate, up, wd),
        [pl.BlockSpec((2, ROWS, ff), lambda i: (0, i, 0))], [jax.ShapeDtypeStruct((2, t, ff), BF16)],
        term, which, collective_id, "hidden_back", cost(2 * t * d * ff, 12 * t * ff),
    )


def product_kernel(a_ref, b_ref, c_ref):
    c_ref[...] = dot(a_ref[...], b_ref[...]).astype(BF16)


def product(a, b, name):
    (m, k), n = a.shape, b.shape[1]
    return pl.pallas_call(
        product_kernel,
        grid=(m // CHUNK,),
        in_specs=[pl.BlockSpec((CHUNK, k), lambda i: (i, 0)), pl.BlockSpec((k, n), lambda i: (0, 0), pipeline_mode=pl.Buffered(1))],
        out_specs=pl.BlockSpec((CHUNK, n), lambda i: (i, 0)),
        out_shape=jax.ShapeDtypeStruct((m, n), BF16),
        compiler_params=params(),
        cost_estimate=cost(2 * m * n * k, 2 * (m * k + k * n + m * n)),
        name=name,
    )(a, b)


def products(a, b, those, steps, term, which, collective_id):
    (m, k), n = a.shape, b.shape[2]
    chunks = n // CHUNK
    grid = len(those) * chunks
    first = those[0]
    return scattering(
        product_kernel, grid, steps,
        [pl.BlockSpec((m, k), lambda i: (0, 0), pipeline_mode=pl.Buffered(1)), pl.BlockSpec((None, k, CHUNK), lambda i: (first + i // chunks, 0, lax.rem(i, chunks)))],
        (a, b),
        [pl.BlockSpec((None, m, CHUNK), lambda i: (i // chunks, 0, lax.rem(i, chunks)))], [jax.ShapeDtypeStruct((len(those), m, n), BF16)],
        term, which, collective_id, "products", cost(2 * m * n * k * len(those), 2 * (m * k + k * n + m * n) * len(those)),
    )


def adamw(total, count, items, layer):
    blocks = [w.shape[1] // 7 if w.shape[1] % 112 == 0 else w.shape[1] // 8 for w, *_ in items]
    steps = [w.shape[1] // block for (w, *_), block in zip(items, blocks, strict=True)]
    starts = [sum(steps[:i]) for i in range(len(items))]
    n_far = sum(len(so_far) for *_, so_far in items)

    def kernel(total_ref, *refs):
        factor = jnp.minimum(1.0, 0.5 * lax.rsqrt(total_ref[0:1, 0:1] / count + 1e-30))
        ins, outs = refs[: 4 * len(items)], refs[4 * len(items) + n_far :]
        for i in range(len(items)):
            w_ref, m_ref, v_ref, g_ref = ins[4 * i : 4 * i + 4]
            new_w_ref, new_m_ref, new_v_ref = outs[3 * i : 3 * i + 3]

            def update(w_ref=w_ref, m_ref=m_ref, v_ref=v_ref, g_ref=g_ref, new_w_ref=new_w_ref, new_m_ref=new_m_ref, new_v_ref=new_v_ref):
                g = g_ref[...].astype(F32) * factor
                m = 0.9 * m_ref[...] + 0.1 * g
                v = 0.95 * v_ref[...] + 0.05 * g * g
                w = w_ref[...].astype(F32)
                new_w_ref[...] = (w - 0.02 * (m * lax.rsqrt(v + 1e-8) + 0.1 * w)).astype(BF16)
                new_m_ref[...] = m
                new_v_ref[...] = v

            if len(items) == 1:
                update()
            else:
                step = pl.program_id(0)
                pl.when((step >= starts[i]) & (step < starts[i] + steps[i]))(update)

    in_specs, args, out_specs, out_shape = [pl.BlockSpec((8, 128), lambda i: (0, 0))], [total], [], []
    for (w, m, v, g, _), block, n, start in zip(items, blocks, steps, starts, strict=True):
        at = lambda i, n=n, start=start: jnp.clip(i - start, 0, n - 1)
        part = pl.BlockSpec((None, block, w.shape[2]), lambda i, at=at: (layer, at(i), 0))
        in_specs += [part, part, part, pl.BlockSpec((block, w.shape[2]), lambda i, at=at: (at(i), 0))]
        args += [w, m, v, g]
        out_specs += [part] * 3
        out_shape += [jax.ShapeDtypeStruct(w.shape, dtype) for dtype in (BF16, F32, F32)]
    far = [one for *_, so_far in items for one in so_far]
    size = sum(w.size for w, *_ in items) // 2
    new = pl.pallas_call(
        kernel,
        grid=(sum(steps),),
        in_specs=in_specs + [pl.BlockSpec(memory_space=pl.ANY)] * n_far,
        out_specs=out_specs,
        out_shape=out_shape,
        input_output_aliases={len(args) + i: i for i in range(n_far)},
        compiler_params=params(),
        cost_estimate=cost(40 * size, 22 * size),
        name="adamw",
    )(*args, *far)
    return [tuple(new[3 * i : 3 * i + 3]) for i in range(len(items))]


def solution(mesh):
    def step(x, dy, *arrays):
        weights, ms, vs = (arrays[i : i + 3] for i in (0, 3, 6))
        x, dy = x[0], dy[0]
        gather = lambda g: lax.all_gather(g, "dp", axis=0, tiled=True)

        at0, gate0, up0, actt0, h1 = forward(x, *weights, 0)
        at1, actt1, by1 = top(h1, dy, *weights, 1)
        shards, squares = [[None] * 3, [None] * 3], []

        def keep(layer, i, shard, square):
            shards[layer][i] = shard
            squares.append(square)

        down1 = product(actt1, dy, "down1")
        pair1, *rest = products(at1, by1, (0, 1), (0, 3), down1, None, 1)
        keep(1, 2, *rest)
        gathered = [None] * 3
        gathered[2] = gather(shards[1][2])
        bh1, *rest = input_back(h1, dy, by1, *weights[:2], 1, pair1, 0, 2)
        keep(1, 0, *rest)
        bh1, gathered[2] = lax.optimization_barrier((bh1, gathered[2]))
        gathered[0] = gather(shards[1][0])
        by0, *rest = hidden_back(bh1, gate0, up0, weights[2], 0, pair1, 1, 3)
        keep(1, 1, *rest)
        by0, gathered[0] = lax.optimization_barrier((by0, gathered[0]))
        gathered[1] = gather(shards[1][1])
        down0 = product(actt0, bh1, "down0")
        gate_term, *rest = products(at0, by0, (0,), (0, 2), down0, None, 4)
        keep(0, 2, *rest)
        gate_term, gathered[1] = lax.optimization_barrier((gate_term, gathered[1]))
        up_term, *rest = products(at0, by0, (1,), (0, 2), gate_term, 0, 5)
        keep(0, 0, *rest)
        shards[0][1], total = last_scatter(up_term, 0, squares, 6)
        held, _ = lax.optimization_barrier((shards[0], total))

        count = sum(w.size for w in weights)
        order = (2, 0, 1)
        items = [(weights[i], ms[i], vs[i], gathered[i], ()) for i in order]
        new = dict(zip(order, adamw(total, count, items, 1), strict=True))
        for i in order:
            (new[i],) = adamw(total, count, [(weights[i], ms[i], vs[i], gather(held[i]), new[i])], 0)
        new = [new[i] for i in range(3)]
        return tuple(one[which] for which in range(3) for one in new)

    return jax.shard_map(
        step,
        mesh=mesh,
        in_specs=(P(("rep", "dp"), None, None),) * 2 + (P(None, None, None),) * 9,
        out_specs=(P("rep", None, None),) * 9,
        check_vma=False,
    )
```

```python
import jax
import jax.numpy as jnp
from jax import lax
from jax.experimental import pallas as pl
from jax.experimental.pallas import tpu as pltpu
from jax.sharding import PartitionSpec as P

BF16, F32 = jnp.bfloat16, jnp.float32
ROWS = 512
CHUNK = 768
VMEM_LIMIT = 62 * 1024 * 1024


def dot(a, b):
    return jnp.dot(a, b, preferred_element_type=F32)


def dot_t(a, b):
    return lax.dot_general(a, b, (((1,), (1,)), ((), ())), preferred_element_type=F32)


def scale_of(h):
    return lax.rsqrt(jnp.mean(h * h, -1, keepdims=True) + 1e-6)


def sigmoid(x):
    return 1.0 / (1.0 + jnp.exp(-x))


def params(n=1):
    return pltpu.CompilerParams(dimension_semantics=("arbitrary",) * n, vmem_limit_bytes=VMEM_LIMIT)


def cost(flops, nbytes):
    return pl.CostEstimate(flops=flops, bytes_accessed=nbytes, transcendentals=0)


def whole(w, layer):
    return pl.BlockSpec((None,) + w.shape[1:], lambda *_: (layer, 0, 0), pipeline_mode=pl.Buffered(1))


def forward_kernel(h_ref, wg_ref, wu_ref, wd_ref, at_ref, gate_ref, up_ref, actt_ref, y_ref):
    h = h_ref[...].astype(F32)
    a = (h * scale_of(h)).astype(BF16)
    at_ref[...] = a.T
    acts = []
    for start in range(0, wg_ref.shape[1], CHUNK):
        cols = pl.ds(start, CHUNK)
        gate, up = dot(a, wg_ref[:, cols]), dot(a, wu_ref[:, cols])
        gate_ref[:, cols] = gate
        up_ref[:, cols] = up
        act = (gate * sigmoid(gate) * up).astype(BF16)
        actt_ref[cols, :] = act.T
        acts.append(act)
    y = dot(jnp.concatenate(acts, 1), wd_ref[...]).astype(BF16)
    y_ref[...] = h_ref[...] + y


def forward(h, wg, wu, wd, layer):
    t, d = h.shape
    ff = wg.shape[2]
    rows = lambda n: pl.BlockSpec((ROWS, n), lambda i: (i, 0))
    cols = lambda n: pl.BlockSpec((n, ROWS), lambda i: (0, i))
    return pl.pallas_call(
        forward_kernel,
        grid=(t // ROWS,),
        in_specs=[rows(d), whole(wg, layer), whole(wu, layer), whole(wd, layer)],
        out_specs=[cols(d), rows(ff), rows(ff), cols(ff), rows(d)],
        out_shape=[
            jax.ShapeDtypeStruct((d, t), BF16),
            jax.ShapeDtypeStruct((t, ff), F32),
            jax.ShapeDtypeStruct((t, ff), F32),
            jax.ShapeDtypeStruct((ff, t), BF16),
            jax.ShapeDtypeStruct((t, d), BF16),
        ],
        compiler_params=params(),
        cost_estimate=cost(6 * t * d * ff, 12 * t * ff),
        name="forward",
    )(h, wg, wu, wd)


def gate_up_back(gate, up, by_act):
    sig = sigmoid(gate)
    silu = gate * sig
    by_gate = by_act * up * (sig + silu * (1.0 - sig))
    return (silu * up).astype(BF16), by_gate.astype(BF16), (by_act * silu).astype(BF16)


def top_kernel(h_ref, dy_ref, wg_ref, wu_ref, wd_ref, at_ref, actt_ref, by_ref):
    h = h_ref[...].astype(F32)
    a = (h * scale_of(h)).astype(BF16)
    at_ref[...] = a.T
    for start in range(0, wg_ref.shape[1], CHUNK):
        cols = pl.ds(start, CHUNK)
        by_act = dot_t(dy_ref[...], wd_ref[cols, :]).astype(BF16).astype(F32)
        act, by_ref[0, :, cols], by_ref[1, :, cols] = gate_up_back(dot(a, wg_ref[:, cols]), dot(a, wu_ref[:, cols]), by_act)
        actt_ref[cols, :] = act.T


def top(h, dy, wg, wu, wd, layer):
    t, d = h.shape
    ff = wg.shape[2]
    rows = lambda n: pl.BlockSpec((ROWS, n), lambda i: (i, 0))
    cols = lambda n: pl.BlockSpec((n, ROWS), lambda i: (0, i))
    return pl.pallas_call(
        top_kernel,
        grid=(t // ROWS,),
        in_specs=[rows(d), rows(d), whole(wg, layer), whole(wu, layer), whole(wd, layer)],
        out_specs=[cols(d), cols(ff), pl.BlockSpec((2, ROWS, ff), lambda i: (0, i, 0))],
        out_shape=[
            jax.ShapeDtypeStruct((d, t), BF16),
            jax.ShapeDtypeStruct((ff, t), BF16),
            jax.ShapeDtypeStruct((2, t, ff), BF16),
        ],
        compiler_params=params(),
        cost_estimate=cost(6 * t * d * ff, 8 * t * ff),
        name="top",
    )(h, dy, wg, wu, wd)


class Scatter:
    def __init__(self, g, send3, kept, mine, got1, send2, got2, local, sent, received):
        self.g, self.send3, self.kept = g, send3, kept
        self.mine, self.got1, self.send2, self.got2 = mine, got1, send2, got2
        self.local, self.sent, self.received = local, sent, received
        me = lax.axis_index("dp")
        self.x, self.y, self.core = me // 4, lax.rem(me // 2, 2), lax.rem(me, 2)
        self.over_core, self.over_x, self.over_y = (self.device(*flip) for flip in ((0, 0, 1), (1, 0, 0), (0, 1, 0)))

    def device(self, x, y, core):
        flip = lambda at, by: 1 - at if by else at
        return {"dp": flip(self.x, x) * 4 + flip(self.y, y) * 2 + flip(self.core, core)}

    def part(self, ref, at, half):
        r, c = half_shape(*ref.shape[1:])
        if r == ref.shape[1]:
            return ref[at, :, half * c : (half + 1) * c]
        return ref[at, half * r : (half + 1) * r, :]

    def own(self, at, half):
        return self.part(self.mine, at, half).astype(F32) + self.part(self.got1, at, half).astype(F32)

    def send(self, src, dst, number, device):
        return pltpu.make_async_remote_copy(
            src_ref=src, dst_ref=dst, send_sem=self.sent.at[number], recv_sem=self.received.at[number],
            device_id=device, device_id_type=pl.DeviceIdType.MESH,
        )

    def fetch(self):
        return pltpu.make_async_copy(self.g.at[:, self.core], self.mine, self.local)

    def first(self):
        r, c = half_shape(*self.got1.shape[1:])
        whole_rows = r == self.got1.shape[1]
        copies = []
        for at in range(4):
            for half in range(2):
                rows, cols = (pl.ds(0, r), pl.ds(half * c, c)) if whole_rows else (pl.ds(half * r, r), pl.ds(0, c))
                copies.append(self.send(self.g.at[at, 1 - self.core, rows, cols], self.got1.at[at, rows, cols], 4 + len(copies), self.over_core))
        return copies

    def pair(self, src, dst, number, devices):
        return [self.send(src.at[half], dst.at[half], number + half, devices[half]) for half in range(2)]

    def second(self):
        return self.pair(self.send2, self.got2, 0, (self.over_x, self.over_y))

    def begin(self, before=None):
        barrier = pltpu.get_barrier_semaphore()
        for device in (self.over_core, self.over_x, self.over_y):
            pl.semaphore_signal(barrier, inc=1, device_id=device, device_id_type=pl.DeviceIdType.MESH)
        pl.semaphore_wait(barrier, 3)
        if before is not None:
            before.start()
        for copy in self.first():
            copy.start()
        self.fetch().start()

    def go_second(self):
        self.fetch().wait()
        for copy in self.first():
            copy.wait()
        for j in range(2):
            self.send2[0, j] = self.own(2 * (1 - self.x) + j, 0).astype(BF16)
            self.send2[1, j] = self.own(2 * j + (1 - self.y), 1).astype(BF16)
        for copy in self.second():
            copy.start()

    def end_second(self):
        for copy in self.second():
            copy.wait()
        x, y = self.x, self.y
        self.send3[0] = (self.own(2 * x + (1 - y), 0) + self.got2[0, 1 - y].astype(F32)).astype(BF16)
        self.send3[1] = (self.own(2 * (1 - x) + y, 1) + self.got2[1, 1 - x].astype(F32)).astype(BF16)
        self.kept[0] = self.own(2 * x + y, 0) + self.got2[0, y].astype(F32)
        self.kept[1] = self.own(2 * x + y, 1) + self.got2[1, x].astype(F32)


class Finish:
    def __init__(self, scatter, send3, kept, out, squares, got3, sent, received):
        self.copies = [
            pltpu.make_async_remote_copy(
                src_ref=send3.at[half], dst_ref=got3.at[half], send_sem=sent.at[half], recv_sem=received.at[half],
                device_id=device, device_id_type=pl.DeviceIdType.MESH,
            )
            for half, device in ((0, scatter.over_y), (1, scatter.over_x))
        ]
        self.kept, self.out, self.squares, self.got3 = kept, out, squares, got3

    def start(self):
        for copy in self.copies:
            copy.start()

    def end(self):
        for copy in self.copies:
            copy.wait()
        r, c = self.out.shape
        hr, hc = half_shape(r, c)
        for half in range(2):
            total = (self.kept[half] + self.got3[half].astype(F32)).astype(BF16)
            square = jnp.sum(jnp.square(total.astype(F32)), 0, keepdims=True)
            if hr == r:
                self.out[:, half * hc : (half + 1) * hc] = total
                self.squares[:, half * hc : (half + 1) * hc] = square
            else:
                self.out[half * hr : (half + 1) * hr, :] = total
                self.squares[...] = square if half == 0 else self.squares[...] + square


def half_shape(r, c):
    return (r, c // 2) if c % 256 == 0 else (r // 2, c)


def scatter_scratch(r, c):
    hr, hc = half_shape(r, c)
    blocks = ((4, r, c), (4, r, c), (2, 2, hr, hc), (2, 2, hr, hc))
    return [pltpu.VMEM(block, BF16) for block in blocks] + [pltpu.SemaphoreType.DMA, pltpu.SemaphoreType.DMA((12,)), pltpu.SemaphoreType.DMA((12,))]


def finish_scratch(r, c):
    return [pltpu.VMEM((2,) + half_shape(r, c), BF16), pltpu.SemaphoreType.DMA((2,)), pltpu.SemaphoreType.DMA((2,))]


def by_device(term):
    r, c = term.shape[-2:]
    return term.reshape(term.shape[:-2] + (4, 2, r // 8, c))


def left_of(r, c):
    return [jax.ShapeDtypeStruct((2,) + half_shape(r, c), dtype) for dtype in (BF16, F32)]


def shard_of(left):
    _, hr, hc = left[0].shape
    return (hr, 2 * hc) if hc % 128 == 0 and hc * 2 % 256 == 0 and hr == 112 else (2 * hr, hc)


def scattering(compute, grid, in_specs, args, out_specs, out_shape, term, which, left, collective_id, name, cost_estimate):
    term = by_device(term)
    r, c = term.shape[-2:]
    n_in, n_out = len(args), len(out_shape)
    fixed = lambda shape: pl.BlockSpec(shape, lambda i: (0,) * len(shape))
    leaves = left_of(r, c)
    in_specs, out_specs, out_shape = list(in_specs), list(out_specs), list(out_shape)
    in_specs += [pl.BlockSpec(memory_space=pl.ANY)]
    out_specs += [fixed(one.shape) for one in leaves]
    out_shape += leaves
    scratch_shapes = scatter_scratch(r, c)
    if left:
        before = shard_of(left)
        in_specs += [pl.BlockSpec(memory_space=pl.ANY), fixed(left[1].shape)]
        out_specs += [fixed(before), fixed((1, before[1]))]
        out_shape += [jax.ShapeDtypeStruct(before, BF16), jax.ShapeDtypeStruct((1, before[1]), F32)]
        scratch_shapes = scratch_shapes + finish_scratch(*before)

    def kernel(*refs):
        refs = list(refs)
        take = lambda n: [refs.pop(0) for _ in range(n)]
        ins, (g,), previous, outs, leaves, done, scratch = (take(n) for n in (n_in, 1, 2 * bool(left), n_out, 2, 2 * bool(left), 7))
        scatter = Scatter(g if which is None else g.at[which], *leaves, *scratch)
        before = Finish(scatter, *previous, *done, *refs) if left else None
        step = pl.program_id(0)
        pl.when(step == 0)(lambda: scatter.begin(before))
        compute(*ins, *outs)
        pl.when(step == 0)(scatter.go_second)
        if left:
            pl.when(step == 1)(before.end)
        pl.when(step == grid - 1)(scatter.end_second)

    results = pl.pallas_call(
        kernel,
        grid=(grid,),
        in_specs=in_specs,
        out_specs=out_specs,
        out_shape=out_shape,
        scratch_shapes=scratch_shapes,
        compiler_params=pltpu.CompilerParams(
            dimension_semantics=("arbitrary",), vmem_limit_bytes=VMEM_LIMIT, collective_id=collective_id, has_side_effects=True
        ),
        cost_estimate=cost_estimate,
        name=name,
    )(*args, term, *left)
    return *results[:n_out], results[n_out : n_out + 2], *results[n_out + 2 :]


def last_scatter(term, which, left, squares, collective_id):
    term = by_device(term)
    r, c = term.shape[-2:]
    before_shape = shard_of(left)

    def kernel(*refs):
        refs = list(refs)
        take = lambda n: [refs.pop(0) for _ in range(n)]
        (g,), previous, others, (out, old, total_ref), scratch, finish1, finish2 = (take(n) for n in (1, 2, len(squares), 3, 7, 3, 3))
        send3, kept, own, own_before, mine, theirs, sent, received = refs
        scatter = Scatter(g.at[which], send3, kept, *scratch)
        before = Finish(scatter, *previous, old, own_before, *finish1)
        last = Finish(scatter, send3, kept, out, own, *finish2)
        scatter.begin(before)
        scatter.go_second()
        before.end()
        rest = sum(jnp.sum(other[...], keepdims=True) for other in (*others, own_before))
        scatter.end_second()
        last.start()
        last.end()
        total = jnp.broadcast_to(rest + jnp.sum(own[...], keepdims=True), (8, 128))
        for i, device in enumerate((scatter.over_core, scatter.over_x, scatter.over_y)):
            mine[i] = total
            copy = pltpu.make_async_remote_copy(
                src_ref=mine.at[i], dst_ref=theirs.at[i], send_sem=sent.at[i], recv_sem=received.at[i],
                device_id=device, device_id_type=pl.DeviceIdType.MESH,
            )
            copy.start()
            copy.wait()
            total = total + theirs[i]
        total_ref[...] = total

    vmem = pl.BlockSpec(memory_space=pltpu.VMEM)
    hbm = pl.BlockSpec(memory_space=pl.ANY)
    return pl.pallas_call(
        kernel,
        in_specs=[hbm, hbm, vmem] + [vmem] * len(squares),
        out_specs=[vmem] * 3,
        out_shape=[jax.ShapeDtypeStruct((r, c), BF16), jax.ShapeDtypeStruct(before_shape, BF16), jax.ShapeDtypeStruct((8, 128), F32)],
        scratch_shapes=scatter_scratch(r, c)
        + finish_scratch(*before_shape)
        + finish_scratch(r, c)
        + [pltpu.VMEM(one.shape, one.dtype) for one in left_of(r, c)]
        + [pltpu.VMEM((1, c), F32), pltpu.VMEM((1, before_shape[1]), F32), pltpu.VMEM((3, 8, 128), F32), pltpu.VMEM((3, 8, 128), F32)]
        + [pltpu.SemaphoreType.DMA((3,)), pltpu.SemaphoreType.DMA((3,))],
        compiler_params=pltpu.CompilerParams(vmem_limit_bytes=VMEM_LIMIT, collective_id=collective_id, has_side_effects=True),
        cost_estimate=cost(2**34, 2**20),
        name="last_scatter",
    )(term, *left, *squares)


def input_back_kernel(h_ref, dy_ref, by_ref, wg_ref, wu_ref, bh_ref):
    by_a = (dot_t(by_ref[0], wg_ref[...]) + dot_t(by_ref[1], wu_ref[...])).astype(BF16).astype(F32)
    h = h_ref[...].astype(F32)
    scale = scale_of(h)
    by_h = scale * (by_a - h * (scale * scale * jnp.mean(by_a * h, -1, keepdims=True)))
    bh_ref[...] = (dy_ref[...].astype(F32) + by_h).astype(BF16)


def input_back(h, dy, by, wg, wu, layer, term, which, left, collective_id):
    t, d = h.shape
    ff = wg.shape[2]
    rows = lambda n: pl.BlockSpec((ROWS, n), lambda i: (i, 0))
    return scattering(
        input_back_kernel, t // ROWS,
        [rows(d), rows(d), pl.BlockSpec((2, ROWS, ff), lambda i: (0, i, 0)), whole(wg, layer), whole(wu, layer)],
        (h, dy, by, wg, wu),
        [rows(d)], [jax.ShapeDtypeStruct((t, d), BF16)],
        term, which, left, collective_id, "input_back", cost(4 * t * d * ff, 6 * t * ff),
    )


def hidden_back_kernel(by_ref, gate_ref, up_ref, wd_ref, out_ref):
    for start in range(0, gate_ref.shape[1], CHUNK):
        cols = pl.ds(start, CHUNK)
        by_act = dot_t(by_ref[...], wd_ref[cols, :]).astype(BF16).astype(F32)
        _, out_ref[0, :, cols], out_ref[1, :, cols] = gate_up_back(gate_ref[:, cols], up_ref[:, cols], by_act)


def hidden_back(by, gate, up, wd, layer, term, which, left, collective_id):
    t, d = by.shape
    ff = gate.shape[1]
    rows = lambda n: pl.BlockSpec((ROWS, n), lambda i: (i, 0))
    return scattering(
        hidden_back_kernel, t // ROWS,
        [rows(d), rows(ff), rows(ff), whole(wd, layer)], (by, gate, up, wd),
        [pl.BlockSpec((2, ROWS, ff), lambda i: (0, i, 0))], [jax.ShapeDtypeStruct((2, t, ff), BF16)],
        term, which, left, collective_id, "hidden_back", cost(2 * t * d * ff, 12 * t * ff),
    )


def product_kernel(a_ref, b_ref, c_ref):
    c_ref[...] = dot(a_ref[...], b_ref[...]).astype(BF16)


def product(a, b, name):
    (m, k), n = a.shape, b.shape[1]
    return pl.pallas_call(
        product_kernel,
        grid=(m // CHUNK,),
        in_specs=[pl.BlockSpec((CHUNK, k), lambda i: (i, 0)), pl.BlockSpec((k, n), lambda i: (0, 0), pipeline_mode=pl.Buffered(1))],
        out_specs=pl.BlockSpec((CHUNK, n), lambda i: (i, 0)),
        out_shape=jax.ShapeDtypeStruct((m, n), BF16),
        compiler_params=params(),
        cost_estimate=cost(2 * m * n * k, 2 * (m * k + k * n + m * n)),
        name=name,
    )(a, b)


def products(a, b, those, term, which, left, collective_id):
    (m, k), n = a.shape, b.shape[2]
    chunks = n // CHUNK
    grid = len(those) * chunks
    first = those[0]
    return scattering(
        product_kernel, grid,
        [pl.BlockSpec((m, k), lambda i: (0, 0), pipeline_mode=pl.Buffered(1)), pl.BlockSpec((None, k, CHUNK), lambda i: (first + i // chunks, 0, lax.rem(i, chunks)))],
        (a, b),
        [pl.BlockSpec((None, m, CHUNK), lambda i: (i // chunks, 0, lax.rem(i, chunks)))], [jax.ShapeDtypeStruct((len(those), m, n), BF16)],
        term, which, left, collective_id, "products", cost(2 * m * n * k * len(those), 2 * (m * k + k * n + m * n) * len(those)),
    )


DEEP = 4


def adamw(total, count, w, m, v, g, layer, so_far):
    _, r, c = w.shape
    block = r // 14 if r % 224 == 0 else r // 16
    n = r // block

    def kernel(total_ref, *refs):
        ins, outs = refs[:4], refs[4 + len(so_far) : 7 + len(so_far)]
        bufs, (arrived, left) = refs[7 + len(so_far) : -2], refs[-2:]
        rows = lambda i: pl.ds(pl.multiple_of(i * block, block), block)

        def fetch(i, slot):
            return [
                pltpu.make_async_copy(ref.at[layer, rows(i)] if k < 3 else ref.at[rows(i)], bufs[k].at[slot], arrived.at[k, slot])
                for k, ref in enumerate(ins)
            ]

        def store(i, slot):
            return [pltpu.make_async_copy(bufs[4 + k].at[slot], ref.at[layer, rows(i)], left.at[k, slot]) for k, ref in enumerate(outs)]

        for i in range(DEEP - 1):
            for copy in fetch(i, i):
                copy.start()
        factor = jnp.minimum(1.0, 0.5 * lax.rsqrt(total_ref[0:1, 0:1] / count + 1e-30))

        def body(i, carry):
            slot = lax.rem(i, DEEP)

            @pl.when(i + DEEP - 1 < n)
            def _():
                for copy in fetch(i + DEEP - 1, lax.rem(i + DEEP - 1, DEEP)):
                    copy.start()

            for copy in fetch(i, slot):
                copy.wait()

            @pl.when(i >= DEEP)
            def _():
                for copy in store(i - DEEP, slot):
                    copy.wait()

            w_ref, m_ref, v_ref, g_ref, new_w_ref, new_m_ref, new_v_ref = (buf.at[slot] for buf in bufs)
            g = g_ref[...].astype(F32) * factor
            m = 0.9 * m_ref[...] + 0.1 * g
            v = 0.95 * v_ref[...] + 0.05 * g * g
            w = w_ref[...].astype(F32)
            new_w_ref[...] = (w - 0.02 * (m * lax.rsqrt(v + 1e-8) + 0.1 * w)).astype(BF16)
            new_m_ref[...] = m
            new_v_ref[...] = v
            for copy in store(i, slot):
                copy.start()
            return carry

        lax.fori_loop(0, n, body, 0)
        for i in range(n - DEEP, n):
            for copy in store(i, i % DEEP):
                copy.wait()

    hbm = pl.BlockSpec(memory_space=pl.ANY)
    types = (BF16, F32, F32, BF16, BF16, F32, F32)
    return pl.pallas_call(
        kernel,
        in_specs=[pl.BlockSpec(memory_space=pltpu.VMEM)] + [hbm] * (4 + len(so_far)),
        out_specs=[hbm] * 3,
        out_shape=[jax.ShapeDtypeStruct(w.shape, dtype) for dtype in (BF16, F32, F32)],
        input_output_aliases={5 + i: i for i in range(len(so_far))},
        scratch_shapes=[pltpu.VMEM((DEEP, block, c), dtype) for dtype in types]
        + [pltpu.SemaphoreType.DMA((4, DEEP)), pltpu.SemaphoreType.DMA((3, DEEP))],
        compiler_params=pltpu.CompilerParams(vmem_limit_bytes=VMEM_LIMIT),
        cost_estimate=cost(2**32, 22 * r * c),
        name="adamw",
    )(total, w, m, v, g, *so_far)


def solution(mesh):
    def step(x, dy, *arrays):
        weights, ms, vs = (arrays[i : i + 3] for i in (0, 3, 6))
        x, dy = x[0], dy[0]
        gather = lambda g: lax.all_gather(g, "dp", axis=0, tiled=True)

        at0, gate0, up0, actt0, h1 = forward(x, *weights, 0)
        at1, actt1, by1 = top(h1, dy, *weights, 1)
        shards, squares, gathered = [[None] * 3, [None] * 3], [], [None] * 3

        def keep(layer, i, shard, square):
            shards[layer][i] = shard
            squares.append(square)

        down1 = product(actt1, dy, "down1")
        pair1, left = products(at1, by1, (0, 1), down1, None, (), 1)
        bh1, left, *done = input_back(h1, dy, by1, *weights[:2], 1, pair1, 0, left, 2)
        keep(1, 2, *done)
        gathered[2] = gather(shards[1][2])
        by0, left, *done = hidden_back(bh1, gate0, up0, weights[2], 0, pair1, 1, left, 3)
        keep(1, 0, *done)
        by0, gathered[2] = lax.optimization_barrier((by0, gathered[2]))
        gathered[0] = gather(shards[1][0])
        down0 = product(actt0, bh1, "down0")
        gate_term, left, *done = products(at0, by0, (0,), down0, None, left, 4)
        keep(1, 1, *done)
        gate_term, gathered[0] = lax.optimization_barrier((gate_term, gathered[0]))
        gathered[1] = gather(shards[1][1])
        up_term, left, *done = products(at0, by0, (1,), gate_term, 0, left, 5)
        keep(0, 2, *done)
        shards[0][1], shards[0][0], total = last_scatter(up_term, 0, left, squares, 6)
        held, _ = lax.optimization_barrier((shards[0], total))

        count = sum(w.size for w in weights)
        order = (2, 0, 1)
        new = {i: adamw(total, count, weights[i], ms[i], vs[i], gathered[i], 1, ()) for i in order}
        for i in order:
            new[i] = adamw(total, count, weights[i], ms[i], vs[i], gather(held[i]), 0, new[i])
        new = [new[i] for i in range(3)]
        return tuple(one[which] for which in range(3) for one in new)

    return jax.shard_map(
        step,
        mesh=mesh,
        in_specs=(P(("rep", "dp"), None, None),) * 2 + (P(None, None, None),) * 9,
        out_specs=(P("rep", None, None),) * 9,
        check_vma=False,
    )
```

```python
import jax
import jax.numpy as jnp
from jax import lax
from jax.experimental import pallas as pl
from jax.experimental.pallas import tpu as pltpu
from jax.sharding import PartitionSpec as P

BF16, F32 = jnp.bfloat16, jnp.float32
ROWS = 512
CHUNK = 768
VMEM_LIMIT = 62 * 1024 * 1024


def dot(a, b):
    return jnp.dot(a, b, preferred_element_type=F32)


def dot_t(a, b):
    return lax.dot_general(a, b, (((1,), (1,)), ((), ())), preferred_element_type=F32)


def scale_of(h):
    return lax.rsqrt(jnp.mean(h * h, -1, keepdims=True) + 1e-6)


def sigmoid(x):
    return 1.0 / (1.0 + jnp.exp(-x))


def params(n=1):
    return pltpu.CompilerParams(dimension_semantics=("arbitrary",) * n, vmem_limit_bytes=VMEM_LIMIT)


def cost(flops, nbytes):
    return pl.CostEstimate(flops=flops, bytes_accessed=nbytes, transcendentals=0)


def whole(w, layer):
    return pl.BlockSpec((None,) + w.shape[1:], lambda *_: (layer, 0, 0), pipeline_mode=pl.Buffered(1))


def forward_kernel(h_ref, wg_ref, wu_ref, wd_ref, at_ref, gate_ref, up_ref, actt_ref, y_ref):
    h = h_ref[...].astype(F32)
    a = (h * scale_of(h)).astype(BF16)
    at_ref[...] = a.T
    acts = []
    for start in range(0, wg_ref.shape[1], CHUNK):
        cols = pl.ds(start, CHUNK)
        gate, up = dot(a, wg_ref[:, cols]), dot(a, wu_ref[:, cols])
        gate_ref[:, cols] = gate
        up_ref[:, cols] = up
        act = (gate * sigmoid(gate) * up).astype(BF16)
        actt_ref[cols, :] = act.T
        acts.append(act)
    y = dot(jnp.concatenate(acts, 1), wd_ref[...]).astype(BF16)
    y_ref[...] = h_ref[...] + y


def forward(h, wg, wu, wd, layer):
    t, d = h.shape
    ff = wg.shape[2]
    rows = lambda n: pl.BlockSpec((ROWS, n), lambda i: (i, 0))
    cols = lambda n: pl.BlockSpec((n, ROWS), lambda i: (0, i))
    return pl.pallas_call(
        forward_kernel,
        grid=(t // ROWS,),
        in_specs=[rows(d), whole(wg, layer), whole(wu, layer), whole(wd, layer)],
        out_specs=[cols(d), rows(ff), rows(ff), cols(ff), rows(d)],
        out_shape=[
            jax.ShapeDtypeStruct((d, t), BF16),
            jax.ShapeDtypeStruct((t, ff), F32),
            jax.ShapeDtypeStruct((t, ff), F32),
            jax.ShapeDtypeStruct((ff, t), BF16),
            jax.ShapeDtypeStruct((t, d), BF16),
        ],
        compiler_params=params(),
        cost_estimate=cost(6 * t * d * ff, 12 * t * ff),
        name="forward",
    )(h, wg, wu, wd)


def gate_up_back(gate, up, by_act):
    sig = sigmoid(gate)
    silu = gate * sig
    by_gate = by_act * up * (sig + silu * (1.0 - sig))
    return (silu * up).astype(BF16), by_gate.astype(BF16), (by_act * silu).astype(BF16)


def top_kernel(h_ref, dy_ref, wg_ref, wu_ref, wd_ref, at_ref, actt_ref, by_ref):
    h = h_ref[...].astype(F32)
    a = (h * scale_of(h)).astype(BF16)
    at_ref[...] = a.T
    for start in range(0, wg_ref.shape[1], CHUNK):
        cols = pl.ds(start, CHUNK)
        by_act = dot_t(dy_ref[...], wd_ref[cols, :]).astype(BF16).astype(F32)
        act, by_ref[0, :, cols], by_ref[1, :, cols] = gate_up_back(dot(a, wg_ref[:, cols]), dot(a, wu_ref[:, cols]), by_act)
        actt_ref[cols, :] = act.T


def top(h, dy, wg, wu, wd, layer):
    t, d = h.shape
    ff = wg.shape[2]
    rows = lambda n: pl.BlockSpec((ROWS, n), lambda i: (i, 0))
    cols = lambda n: pl.BlockSpec((n, ROWS), lambda i: (0, i))
    return pl.pallas_call(
        top_kernel,
        grid=(t // ROWS,),
        in_specs=[rows(d), rows(d), whole(wg, layer), whole(wu, layer), whole(wd, layer)],
        out_specs=[cols(d), cols(ff), pl.BlockSpec((2, ROWS, ff), lambda i: (0, i, 0))],
        out_shape=[
            jax.ShapeDtypeStruct((d, t), BF16),
            jax.ShapeDtypeStruct((ff, t), BF16),
            jax.ShapeDtypeStruct((2, t, ff), BF16),
        ],
        compiler_params=params(),
        cost_estimate=cost(6 * t * d * ff, 8 * t * ff),
        name="top",
    )(h, dy, wg, wu, wd)


class Scatter:
    def __init__(self, g, send3, kept, mine, got1, send2, got2, local, sent, received):
        self.g, self.send3, self.kept = g, send3, kept
        self.mine, self.got1, self.send2, self.got2 = mine, got1, send2, got2
        self.local, self.sent, self.received = local, sent, received
        me = lax.axis_index("dp")
        self.x, self.y, self.core = me // 4, lax.rem(me // 2, 2), lax.rem(me, 2)
        self.over_core, self.over_x, self.over_y = (self.device(*flip) for flip in ((0, 0, 1), (1, 0, 0), (0, 1, 0)))

    def device(self, x, y, core):
        flip = lambda at, by: 1 - at if by else at
        return {"dp": flip(self.x, x) * 4 + flip(self.y, y) * 2 + flip(self.core, core)}

    def part(self, ref, at, half):
        r, c = half_shape(*ref.shape[1:])
        if r == ref.shape[1]:
            return ref[at, :, half * c : (half + 1) * c]
        return ref[at, half * r : (half + 1) * r, :]

    def own(self, at, half):
        return self.part(self.mine, at, half).astype(F32) + self.part(self.got1, at, half).astype(F32)

    def send(self, src, dst, number, device):
        return pltpu.make_async_remote_copy(
            src_ref=src, dst_ref=dst, send_sem=self.sent.at[number], recv_sem=self.received.at[number],
            device_id=device, device_id_type=pl.DeviceIdType.MESH,
        )

    def fetch(self):
        return pltpu.make_async_copy(self.g.at[:, self.core], self.mine, self.local)

    def first(self):
        r, c = half_shape(*self.got1.shape[1:])
        whole_rows = r == self.got1.shape[1]
        copies = []
        for at in range(4):
            for half in range(2):
                rows, cols = (pl.ds(0, r), pl.ds(half * c, c)) if whole_rows else (pl.ds(half * r, r), pl.ds(0, c))
                copies.append(self.send(self.g.at[at, 1 - self.core, rows, cols], self.got1.at[at, rows, cols], 4 + len(copies), self.over_core))
        return copies

    def pair(self, src, dst, number, devices):
        return [self.send(src.at[half], dst.at[half], number + half, devices[half]) for half in range(2)]

    def second(self):
        return self.pair(self.send2, self.got2, 0, (self.over_x, self.over_y))

    def begin(self, before=None, devices=None):
        barrier = pltpu.get_barrier_semaphore()
        devices = (self.over_core, self.over_x, self.over_y) if devices is None else devices
        for device in devices:
            pl.semaphore_signal(barrier, inc=1, device_id=device, device_id_type=pl.DeviceIdType.MESH)
        pl.semaphore_wait(barrier, len(devices))
        if before is not None:
            before.start()
        for copy in self.first():
            copy.start()
        self.fetch().start()

    def go_second(self):
        self.fetch().wait()
        for copy in self.first():
            copy.wait()
        for j in range(2):
            self.send2[0, j] = self.own(2 * (1 - self.x) + j, 0).astype(BF16)
            self.send2[1, j] = self.own(2 * j + (1 - self.y), 1).astype(BF16)
        for copy in self.second():
            copy.start()

    def end_second(self):
        for copy in self.second():
            copy.wait()
        x, y = self.x, self.y
        self.send3[0] = (self.own(2 * x + (1 - y), 0) + self.got2[0, 1 - y].astype(F32)).astype(BF16)
        self.send3[1] = (self.own(2 * (1 - x) + y, 1) + self.got2[1, 1 - x].astype(F32)).astype(BF16)
        self.kept[0] = self.own(2 * x + y, 0) + self.got2[0, y].astype(F32)
        self.kept[1] = self.own(2 * x + y, 1) + self.got2[1, x].astype(F32)


class Finish:
    def __init__(self, scatter, send3, kept, out, squares, got3, sent, received):
        self.copies = [
            pltpu.make_async_remote_copy(
                src_ref=send3.at[half], dst_ref=got3.at[half], send_sem=sent.at[half], recv_sem=received.at[half],
                device_id=device, device_id_type=pl.DeviceIdType.MESH,
            )
            for half, device in ((0, scatter.over_y), (1, scatter.over_x))
        ]
        self.kept, self.out, self.squares, self.got3 = kept, out, squares, got3

    def start(self):
        for copy in self.copies:
            copy.start()

    def end(self):
        for copy in self.copies:
            copy.wait()
        r, c = self.out.shape
        hr, hc = half_shape(r, c)
        for half in range(2):
            total = (self.kept[half] + self.got3[half].astype(F32)).astype(BF16)
            square = jnp.sum(jnp.square(total.astype(F32)), 0, keepdims=True)
            if hr == r:
                self.out[:, half * hc : (half + 1) * hc] = total
                self.squares[:, half * hc : (half + 1) * hc] = square
            else:
                self.out[half * hr : (half + 1) * hr, :] = total
                self.squares[...] = square if half == 0 else self.squares[...] + square


def half_shape(r, c):
    return (r, c // 2) if c % 256 == 0 else (r // 2, c)


def scatter_scratch(r, c):
    hr, hc = half_shape(r, c)
    blocks = ((4, r, c), (4, r, c), (2, 2, hr, hc), (2, 2, hr, hc))
    return [pltpu.VMEM(block, BF16) for block in blocks] + [pltpu.SemaphoreType.DMA, pltpu.SemaphoreType.DMA((12,)), pltpu.SemaphoreType.DMA((12,))]


def finish_scratch(r, c):
    return [pltpu.VMEM((2,) + half_shape(r, c), BF16), pltpu.SemaphoreType.DMA((2,)), pltpu.SemaphoreType.DMA((2,))]


def by_device(term):
    r, c = term.shape[-2:]
    return term.reshape(term.shape[:-2] + (4, 2, r // 8, c))


def left_of(r, c):
    return [jax.ShapeDtypeStruct((2,) + half_shape(r, c), dtype) for dtype in (BF16, F32)]


def shard_of(left):
    _, hr, hc = left[0].shape
    return (hr, 2 * hc) if hc % 128 == 0 and hc * 2 % 256 == 0 and hr == 112 else (2 * hr, hc)


def scattering(compute, grid, in_specs, args, out_specs, out_shape, term, which, left, collective_id, name, cost_estimate):
    term = by_device(term)
    r, c = term.shape[-2:]
    n_in, n_out = len(args), len(out_shape)
    fixed = lambda shape: pl.BlockSpec(shape, lambda i: (0,) * len(shape))
    leaves = left_of(r, c)
    in_specs, out_specs, out_shape = list(in_specs), list(out_specs), list(out_shape)
    in_specs += [pl.BlockSpec(memory_space=pl.ANY)]
    out_specs += [fixed(one.shape) for one in leaves]
    out_shape += leaves
    scratch_shapes = scatter_scratch(r, c)
    if left:
        before = shard_of(left)
        in_specs += [pl.BlockSpec(memory_space=pl.ANY), fixed(left[1].shape)]
        out_specs += [fixed(before), fixed((1, before[1]))]
        out_shape += [jax.ShapeDtypeStruct(before, BF16), jax.ShapeDtypeStruct((1, before[1]), F32)]
        scratch_shapes = scratch_shapes + finish_scratch(*before)

    def kernel(*refs):
        refs = list(refs)
        take = lambda n: [refs.pop(0) for _ in range(n)]
        ins, (g,), previous, outs, leaves, done, scratch = (take(n) for n in (n_in, 1, 2 * bool(left), n_out, 2, 2 * bool(left), 7))
        scatter = Scatter(g if which is None else g.at[which], *leaves, *scratch)
        before = Finish(scatter, *previous, *done, *refs) if left else None
        step = pl.program_id(0)
        pl.when(step == 0)(lambda: scatter.begin(before))
        compute(*ins, *outs)
        pl.when(step == 0)(scatter.go_second)
        if left:
            pl.when(step == 1)(before.end)
        pl.when(step == grid - 1)(scatter.end_second)

    results = pl.pallas_call(
        kernel,
        grid=(grid,),
        in_specs=in_specs,
        out_specs=out_specs,
        out_shape=out_shape,
        scratch_shapes=scratch_shapes,
        compiler_params=pltpu.CompilerParams(
            dimension_semantics=("arbitrary",), vmem_limit_bytes=VMEM_LIMIT, collective_id=collective_id, has_side_effects=True
        ),
        cost_estimate=cost_estimate,
        name=name,
    )(*args, term, *left)
    return *results[:n_out], results[n_out : n_out + 2], *results[n_out + 2 :]


def last_scatter(term, which, left, squares, collective_id):
    term = by_device(term)
    r, c = term.shape[-2:]
    before_shape = shard_of(left)

    def kernel(*refs):
        refs = list(refs)
        take = lambda n: [refs.pop(0) for _ in range(n)]
        (g,), previous, others, (out, old, total_ref), scratch, finish1, finish2 = (take(n) for n in (1, 2, len(squares), 3, 7, 3, 3))
        send3, kept, own, own_before, mine, theirs, sent, received = refs
        scatter = Scatter(g.at[which], send3, kept, *scratch)
        before = Finish(scatter, *previous, old, own_before, *finish1)
        last = Finish(scatter, send3, kept, out, own, *finish2)
        me = lax.axis_index("dp")
        everybody = [{"dp": lax.rem(me + by, 8)} for by in range(1, 8)]
        scatter.begin(before, everybody)
        scatter.go_second()
        before.end()
        rest = sum(jnp.sum(other[...], keepdims=True) for other in (*others, own_before))
        scatter.end_second()
        last.start()
        last.end()
        mine[...] = jnp.broadcast_to(rest + jnp.sum(own[...], keepdims=True), (8, 128))
        copies = [
            pltpu.make_async_remote_copy(
                src_ref=mine, dst_ref=theirs.at[me], send_sem=sent.at[i], recv_sem=received.at[i],
                device_id=device, device_id_type=pl.DeviceIdType.MESH,
            )
            for i, device in enumerate(everybody)
        ]
        for copy in copies:
            copy.start()
        theirs[me] = mine[...]
        for copy in copies:
            copy.wait()
        total = theirs[0]
        for i in range(1, 8):
            total = total + theirs[i]
        total_ref[...] = total

    vmem = pl.BlockSpec(memory_space=pltpu.VMEM)
    hbm = pl.BlockSpec(memory_space=pl.ANY)
    return pl.pallas_call(
        kernel,
        in_specs=[hbm, hbm, vmem] + [vmem] * len(squares),
        out_specs=[vmem] * 3,
        out_shape=[jax.ShapeDtypeStruct((r, c), BF16), jax.ShapeDtypeStruct(before_shape, BF16), jax.ShapeDtypeStruct((8, 128), F32)],
        scratch_shapes=scatter_scratch(r, c)
        + finish_scratch(*before_shape)
        + finish_scratch(r, c)
        + [pltpu.VMEM(one.shape, one.dtype) for one in left_of(r, c)]
        + [pltpu.VMEM((1, c), F32), pltpu.VMEM((1, before_shape[1]), F32), pltpu.VMEM((8, 128), F32), pltpu.VMEM((8, 8, 128), F32)]
        + [pltpu.SemaphoreType.DMA((7,)), pltpu.SemaphoreType.DMA((7,))],
        compiler_params=pltpu.CompilerParams(vmem_limit_bytes=VMEM_LIMIT, collective_id=collective_id, has_side_effects=True),
        cost_estimate=cost(2**34, 2**20),
        name="last_scatter",
    )(term, *left, *squares)


def input_back_kernel(h_ref, dy_ref, by_ref, wg_ref, wu_ref, bh_ref):
    by_a = (dot_t(by_ref[0], wg_ref[...]) + dot_t(by_ref[1], wu_ref[...])).astype(BF16).astype(F32)
    h = h_ref[...].astype(F32)
    scale = scale_of(h)
    by_h = scale * (by_a - h * (scale * scale * jnp.mean(by_a * h, -1, keepdims=True)))
    bh_ref[...] = (dy_ref[...].astype(F32) + by_h).astype(BF16)


def input_back(h, dy, by, wg, wu, layer, term, which, left, collective_id):
    t, d = h.shape
    ff = wg.shape[2]
    rows = lambda n: pl.BlockSpec((ROWS, n), lambda i: (i, 0))
    return scattering(
        input_back_kernel, t // ROWS,
        [rows(d), rows(d), pl.BlockSpec((2, ROWS, ff), lambda i: (0, i, 0)), whole(wg, layer), whole(wu, layer)],
        (h, dy, by, wg, wu),
        [rows(d)], [jax.ShapeDtypeStruct((t, d), BF16)],
        term, which, left, collective_id, "input_back", cost(4 * t * d * ff, 6 * t * ff),
    )


def hidden_back_kernel(by_ref, gate_ref, up_ref, wd_ref, out_ref):
    for start in range(0, gate_ref.shape[1], CHUNK):
        cols = pl.ds(start, CHUNK)
        by_act = dot_t(by_ref[...], wd_ref[cols, :]).astype(BF16).astype(F32)
        _, out_ref[0, :, cols], out_ref[1, :, cols] = gate_up_back(gate_ref[:, cols], up_ref[:, cols], by_act)


def hidden_back(by, gate, up, wd, layer, term, which, left, collective_id):
    t, d = by.shape
    ff = gate.shape[1]
    rows = lambda n: pl.BlockSpec((ROWS, n), lambda i: (i, 0))
    return scattering(
        hidden_back_kernel, t // ROWS,
        [rows(d), rows(ff), rows(ff), whole(wd, layer)], (by, gate, up, wd),
        [pl.BlockSpec((2, ROWS, ff), lambda i: (0, i, 0))], [jax.ShapeDtypeStruct((2, t, ff), BF16)],
        term, which, left, collective_id, "hidden_back", cost(2 * t * d * ff, 12 * t * ff),
    )


def product_kernel(a_ref, b_ref, c_ref):
    c_ref[...] = dot(a_ref[...], b_ref[...]).astype(BF16)


def product(a, b, name):
    (m, k), n = a.shape, b.shape[1]
    return pl.pallas_call(
        product_kernel,
        grid=(m // CHUNK,),
        in_specs=[pl.BlockSpec((CHUNK, k), lambda i: (i, 0)), pl.BlockSpec((k, n), lambda i: (0, 0), pipeline_mode=pl.Buffered(1))],
        out_specs=pl.BlockSpec((CHUNK, n), lambda i: (i, 0)),
        out_shape=jax.ShapeDtypeStruct((m, n), BF16),
        compiler_params=params(),
        cost_estimate=cost(2 * m * n * k, 2 * (m * k + k * n + m * n)),
        name=name,
    )(a, b)


def products(a, b, those, term, which, left, collective_id):
    (m, k), n = a.shape, b.shape[2]
    chunks = n // CHUNK
    grid = len(those) * chunks
    first = those[0]
    return scattering(
        product_kernel, grid,
        [pl.BlockSpec((m, k), lambda i: (0, 0), pipeline_mode=pl.Buffered(1)), pl.BlockSpec((None, k, CHUNK), lambda i: (first + i // chunks, 0, lax.rem(i, chunks)))],
        (a, b),
        [pl.BlockSpec((None, m, CHUNK), lambda i: (i // chunks, 0, lax.rem(i, chunks)))], [jax.ShapeDtypeStruct((len(those), m, n), BF16)],
        term, which, left, collective_id, "products", cost(2 * m * n * k * len(those), 2 * (m * k + k * n + m * n) * len(those)),
    )


DEEP = 4


class Stream:
    def __init__(self, layer, block, ins, outs, bufs, arrived, left):
        self.layer, self.block, self.ins, self.outs, self.bufs, self.arrived, self.left = layer, block, ins, outs, bufs, arrived, left
        self.n = ins[3].shape[0] // block

    def rows(self, i):
        return pl.ds(pl.multiple_of(i * self.block, self.block), self.block)

    def fetch(self, i, slot):
        refs = [ref.at[self.layer, self.rows(i)] if k < 3 else ref.at[self.rows(i)] for k, ref in enumerate(self.ins)]
        return [pltpu.make_async_copy(ref, self.bufs[k].at[slot], self.arrived.at[k, slot]) for k, ref in enumerate(refs)]

    def store(self, i, slot):
        return [pltpu.make_async_copy(self.bufs[4 + k].at[slot], ref.at[self.layer, self.rows(i)], self.left.at[k, slot]) for k, ref in enumerate(self.outs)]

    def begin(self):
        for i in range(DEEP - 1):
            for copy in self.fetch(i, i):
                copy.start()

    def run(self, factor):
        def body(i, carry):
            slot = lax.rem(i, DEEP)

            @pl.when(i + DEEP - 1 < self.n)
            def _():
                for copy in self.fetch(i + DEEP - 1, lax.rem(i + DEEP - 1, DEEP)):
                    copy.start()

            for copy in self.fetch(i, slot):
                copy.wait()

            @pl.when(i >= DEEP)
            def _():
                for copy in self.store(i - DEEP, slot):
                    copy.wait()

            w_ref, m_ref, v_ref, g_ref, new_w_ref, new_m_ref, new_v_ref = (buf.at[slot] for buf in self.bufs)
            g = g_ref[...].astype(F32) * factor
            m = 0.9 * m_ref[...] + 0.1 * g
            v = 0.95 * v_ref[...] + 0.05 * g * g
            w = w_ref[...].astype(F32)
            new_w_ref[...] = (w - 0.02 * (m * lax.rsqrt(v + 1e-8) + 0.1 * w)).astype(BF16)
            new_m_ref[...] = m
            new_v_ref[...] = v
            for copy in self.store(i, slot):
                copy.start()
            return carry

        lax.fori_loop(0, self.n, body, 0)

    def end(self):
        for i in range(self.n - DEEP, self.n):
            for copy in self.store(i, i % DEEP):
                copy.wait()


def adamw(total, count, items, layer):
    far = [one for *_, so_far in items for one in so_far]
    blocks = [w.shape[1] // 14 if w.shape[1] % 224 == 0 else w.shape[1] // 16 for w, *_ in items]

    def kernel(total_ref, *refs):
        refs = list(refs)
        take = lambda n: [refs.pop(0) for _ in range(n)]
        ins, _, outs = [take(4) for _ in items], take(len(far)), [take(3) for _ in items]
        streams = [Stream(layer, block, i, o, take(7), *take(2)) for block, i, o in zip(blocks, ins, outs, strict=True)]
        for stream in streams:
            stream.begin()
        factor = jnp.minimum(1.0, 0.5 * lax.rsqrt(total_ref[0:1, 0:1] / count + 1e-30))
        for stream in streams:
            stream.run(factor)
        for stream in streams:
            stream.end()

    hbm = pl.BlockSpec(memory_space=pl.ANY)
    scratch_shapes = []
    for (w, *_), block in zip(items, blocks, strict=True):
        scratch_shapes += [pltpu.VMEM((DEEP, block, w.shape[2]), dtype) for dtype in (BF16, F32, F32, BF16, BF16, F32, F32)]
        scratch_shapes += [pltpu.SemaphoreType.DMA((4, DEEP)), pltpu.SemaphoreType.DMA((3, DEEP))]
    size = sum(w.size for w, *_ in items) // 2
    new = pl.pallas_call(
        kernel,
        in_specs=[pl.BlockSpec(memory_space=pltpu.VMEM)] + [hbm] * (4 * len(items) + len(far)),
        out_specs=[hbm] * (3 * len(items)),
        out_shape=[jax.ShapeDtypeStruct(w.shape, dtype) for w, *_ in items for dtype in (BF16, F32, F32)],
        input_output_aliases={1 + 4 * len(items) + i: i for i in range(len(far))},
        scratch_shapes=scratch_shapes,
        compiler_params=pltpu.CompilerParams(vmem_limit_bytes=VMEM_LIMIT),
        cost_estimate=cost(2**32 * len(items), 22 * size),
        name="adamw",
    )(total, *[one for item in items for one in item[:4]], *far)
    return [tuple(new[3 * i : 3 * i + 3]) for i in range(len(items))]


def solution(mesh):
    def step(x, dy, *arrays):
        weights, ms, vs = (arrays[i : i + 3] for i in (0, 3, 6))
        x, dy = x[0], dy[0]
        gather = lambda g: lax.all_gather(g, "dp", axis=0, tiled=True)

        at0, gate0, up0, actt0, h1 = forward(x, *weights, 0)
        at1, actt1, by1 = top(h1, dy, *weights, 1)
        shards, squares, gathered = [[None] * 3, [None] * 3], [], [None] * 3

        def keep(layer, i, shard, square):
            shards[layer][i] = shard
            squares.append(square)

        down1 = product(actt1, dy, "down1")
        pair1, left = products(at1, by1, (0, 1), down1, None, (), 1)
        bh1, left, *done = input_back(h1, dy, by1, *weights[:2], 1, pair1, 0, left, 2)
        keep(1, 2, *done)
        gathered[2] = gather(shards[1][2])
        by0, left, *done = hidden_back(bh1, gate0, up0, weights[2], 0, pair1, 1, left, 3)
        keep(1, 0, *done)
        by0, gathered[2] = lax.optimization_barrier((by0, gathered[2]))
        gathered[0] = gather(shards[1][0])
        down0 = product(actt0, bh1, "down0")
        gate_term, left, *done = products(at0, by0, (0,), down0, None, left, 4)
        keep(1, 1, *done)
        gate_term, gathered[0] = lax.optimization_barrier((gate_term, gathered[0]))
        gathered[1] = gather(shards[1][1])
        up_term, left, *done = products(at0, by0, (1,), gate_term, 0, left, 5)
        keep(0, 2, *done)
        shards[0][1], shards[0][0], total = last_scatter(up_term, 0, left, squares, 6)
        (*held, _) = lax.optimization_barrier((*shards[0][:2], total))
        held.append(shards[0][2])

        count = sum(w.size for w in weights)
        order = (2, 0, 1)
        items = [(weights[i], ms[i], vs[i], gathered[i], ()) for i in order]
        new = dict(zip(order, adamw(total, count, items, 1), strict=True))
        for i in order:
            (new[i],) = adamw(total, count, [(weights[i], ms[i], vs[i], gather(held[i]), new[i])], 0)
        new = [new[i] for i in range(3)]
        return tuple(one[which] for which in range(3) for one in new)

    return jax.shard_map(
        step,
        mesh=mesh,
        in_specs=(P(("rep", "dp"), None, None),) * 2 + (P(None, None, None),) * 9,
        out_specs=(P("rep", None, None),) * 9,
        check_vma=False,
    )
```
